64 devices in a mesh: tasks: 4 (over x, y), group: 16 (over z, core).
Axes of the slice: x: 2, y: 2, z: 8, core: 2. Of those that a mesh axis runs over, the one named last changes fastest.
The devices are a block of a 4x4x8 slice.
Arguments:
- points: bfloat16 [131072, 512], P(('tasks', 'group')), parts along dimension 0
- vectors: bfloat16 [131072, 16], P(('tasks', 'group')), parts along dimension 0
- lengthscale: float32 [1], replicated
- outscale: float32 [1], replicated
Outputs:
- output: float32 [131072, 16], P(('tasks', 'group')), parts along dimension 0
There are 4 independent parts. The reference program is written for one: setup_inputs(seed, part) draws one part's arguments, and reference() takes and returns one part's arrays. A program takes and returns all parts, laid end to end along the dimension named above; an argument that names none is the same for every part.
All inputs are finite; a program needn't handle non-finite values.
Results may differ from the reference program's by a relative error of at most 0.001.
Values are sent between devices in bfloat16 or wider.
A program may use at most 768 MiB of HBM per device.

```python
import jax
import jax.numpy as jnp
from jax import lax

NUM_POINTS = 32768
FEAT_DIM = 512
NUM_RHS = 16
QUERY_BLOCK = 256
LATENT_DIM = 8


def setup_inputs(seed: int = 0, part: int = 0) -> dict:
    base_key = jax.random.key(seed)
    part_key = jax.random.fold_in(base_key, part)
    key_lat, key_mix, key_noise, key_rhs = jax.random.split(part_key, 4)
    key_ell, key_scale = jax.random.split(jax.random.key(seed + 29), 2)
    latent = jax.random.normal(key_lat, (NUM_POINTS, LATENT_DIM), jnp.float32)
    mixing = jax.random.normal(key_mix, (LATENT_DIM, FEAT_DIM), jnp.float32) * FEAT_DIM ** -0.5
    noise = jax.random.normal(key_noise, (NUM_POINTS, FEAT_DIM), jnp.float32) * (0.3 * FEAT_DIM ** -0.5)
    points = (jnp.dot(latent, mixing) + noise).astype(jnp.bfloat16)
    vectors = (jax.random.normal(key_rhs, (NUM_POINTS, NUM_RHS), jnp.float32) * NUM_POINTS ** -0.5).astype(jnp.bfloat16)
    lengthscale = jax.random.uniform(key_ell, (1,), jnp.float32, 2.4, 3.1)
    outscale = jax.random.uniform(key_scale, (1,), jnp.float32, 0.6, 1.6)
    return {'points': points, 'vectors': vectors, 'lengthscale': lengthscale, 'outscale': outscale}


def reference(points, vectors, lengthscale, outscale):
    sq_norm = jnp.sum(jnp.square(points.astype(jnp.float32)), axis=1)
    two_ell_sq = 2.0 * jnp.square(lengthscale[0])
    query_pts = points.reshape(NUM_POINTS // QUERY_BLOCK, QUERY_BLOCK, FEAT_DIM)
    query_norm = sq_norm.reshape(NUM_POINTS // QUERY_BLOCK, QUERY_BLOCK)

    def one_block(block_pair):
        block_pts, block_norm = block_pair
        gram_mat = jnp.dot(block_pts, points.T, preferred_element_type=jnp.float32)
        sq_dist = jnp.maximum(block_norm[:, None] + sq_norm[None, :] - 2.0 * gram_mat, 0.0)
        kern_blk = (outscale[0] * jnp.exp(-sq_dist / two_ell_sq)).astype(jnp.bfloat16)
        return jnp.dot(kern_blk, vectors, preferred_element_type=jnp.float32)

    result = lax.map(one_block, (query_pts, query_norm))
    return result.reshape(NUM_POINTS, NUM_RHS)
```

```python
import jax
import jax.numpy as jnp
from jax import lax
from jax.experimental import pallas as pl
from jax.experimental.pallas import tpu as pltpu
from jax.sharding import PartitionSpec as P

MESH = pl.DeviceIdType.MESH
NT = (((1,), (1,)), ((), ()))
NN = (((1,), (0,)), ((), ()))
LOG2E = 1.4426950408889634
M2, M1, OWN, P1, P2, T0, T1, TF = range(8)
R_OWN, R_T0, R_M1, R_P1, R_T1, R_FAR = range(6)
C_M1, C_P1, C_M2, C_P2, C_T1, C_TF, C_T0 = range(7)
N_CHUNK = 8
ROWS = 1024


def dot(a, b, dims):
    return lax.dot_general(a, b, dims, preferred_element_type=jnp.float32)


def kernel(n_group, ell_ref, s_ref, x_ref, v_ref, y_ref, xs, vt, nrm, arep, acc, rx,
           load_sem, x_send, x_recv, v_send, v_recv, n_send, n_recv, t0_sem, r_send, r_recv):
    n_rows = x_ref.shape[0]
    chunk = n_rows // N_CHUNK
    n_chip = n_group // 2
    me = lax.axis_index('group')
    chip, core = me // 2, me % 2
    up = ((chip + 1) % n_chip) * 2 + core
    down = ((chip + n_chip - 1) % n_chip) * 2 + core
    partner = chip * 2 + 1 - core
    far_half = chip // (n_chip // 2)
    far_row = M2 + (P2 - M2) * far_half
    far_col = P2 - (P2 - M2) * far_half
    far_base = pl.multiple_of(far_half * ROWS, ROWS)

    def rows_of(j):
        return pl.ds(pl.multiple_of(j * chunk, chunk), chunk)

    def flip(j):
        return (j + N_CHUNK // 2) % N_CHUNK

    SRC = {C_M1: OWN, C_P1: OWN, C_M2: M1, C_P2: P1, C_T1: P1, C_TF: far_col, C_T0: OWN}
    DST = {C_M1: M1, C_P1: P1, C_M2: M2, C_P2: P2, C_T1: T1, C_TF: TF, C_T0: T0}
    TO = {C_M1: up, C_P1: down, C_M2: up, C_P2: down, C_T1: partner, C_TF: partner, C_T0: partner}

    def x_copy(c, j):
        return pltpu.make_async_remote_copy(
            src_ref=xs.at[SRC[c], rows_of(j)], dst_ref=xs.at[DST[c], rows_of(j)],
            send_sem=x_send.at[c, j], recv_sem=x_recv.at[c, j],
            device_id={'group': TO[c]}, device_id_type=MESH)

    def t0_copy():
        return pltpu.make_async_remote_copy(
            src_ref=xs.at[OWN], dst_ref=xs.at[T0], send_sem=t0_sem.at[0], recv_sem=t0_sem.at[1],
            device_id={'group': partner}, device_id_type=MESH)

    def v_copy(c):
        src = v_ref if c in (C_M1, C_P1, C_T0) else vt.at[SRC[c]]
        return pltpu.make_async_remote_copy(
            src_ref=src, dst_ref=vt.at[DST[c]], send_sem=v_send.at[c], recv_sem=v_recv.at[c],
            device_id={'group': TO[c]}, device_id_type=MESH)

    def n_copy(c):
        return pltpu.make_async_remote_copy(
            src_ref=nrm.at[SRC[c]], dst_ref=nrm.at[DST[c]], send_sem=n_send.at[c], recv_sem=n_recv.at[c],
            device_id={'group': TO[c]}, device_id_type=MESH)

    def r_copy(src, i, to):
        return pltpu.make_async_remote_copy(
            src_ref=acc.at[src], dst_ref=rx.at[i], send_sem=r_send.at[i], recv_sem=r_recv.at[i],
            device_id={'group': to}, device_id_type=MESH)

    def load(j):
        return pltpu.make_async_copy(x_ref.at[rows_of(j)], xs.at[OWN, rows_of(j)], load_sem.at[j])

    for j in range(N_CHUNK):
        load(j).start()
    barrier = pltpu.get_barrier_semaphore()
    for peer in (up, down, partner):
        pl.semaphore_signal(barrier, inc=1, device_id={'group': peer}, device_id_type=MESH)
    pl.semaphore_wait(barrier, 3)
    for c in (C_M1, C_P1, C_T0):
        v_copy(c).start()
    for j in range(N_CHUNK):
        load(j).wait()
    for j in range(N_CHUNK):
        x_copy(C_M1, j).start()
        x_copy(C_P1, flip(j)).start()
    t0_copy().start()

    ell = jnp.full((1, 128), ell_ref[0], jnp.float32)
    coef = LOG2E / (2.0 * jnp.square(ell))
    top = LOG2E * jnp.log(jnp.full((1, 128), s_ref[0], jnp.float32))
    coef_2 = jnp.concatenate([coef, coef], axis=1)
    two_coef = 2.0 * coef_2
    top_2 = jnp.concatenate([top, top], axis=1)

    acc[...] = jnp.zeros_like(acc)
    vt[OWN] = v_ref[...]

    def own_norms(b, _):
        rows = pl.ds(pl.multiple_of(b * 128, 128), 128)
        part = jnp.sum(jnp.square(xs[OWN, rows, :].astype(jnp.float32)), axis=1, keepdims=True)
        part = jnp.broadcast_to(part, (128, 128))
        arep[R_OWN, rows, :] = part * coef - top
        nrm[OWN, :, rows] = part.T[0:1, :]
        return 0

    lax.fori_loop(0, n_rows // 128, own_norms, 0)

    def column_norms(slot, to, start, n):
        def one(b, _):
            src = pl.ds(pl.multiple_of(start + b * 128, 128), 128)
            dst = pl.ds(pl.multiple_of(b * 128, 128), 128)
            row = jnp.broadcast_to(nrm[slot, :, src], (128, 128))
            arep[to, dst, :] = row.T * coef - top
            return 0
        lax.fori_loop(0, n // 128, one, 0)

    def unit(row_slot, row_start, rep_slot, rep_start, col_slot, j, want_row):
        rows = pl.ds(pl.multiple_of(row_start, ROWS), ROWS)
        reps = pl.ds(pl.multiple_of(rep_start, ROWS), ROWS)
        cols = rows_of(j)
        gram = dot(xs[row_slot, rows, :], xs[col_slot, cols, :], NT)
        shift = arep[rep_slot, reps, :]
        shift = jnp.concatenate([shift, shift], axis=1)
        expo = jnp.minimum(gram * two_coef - shift - nrm[col_slot, :, cols] * coef_2, top_2)
        kern = jnp.exp2(expo).astype(jnp.bfloat16)
        acc[col_slot, :, cols] += dot(vt[row_slot, :, rows], kern, NN)
        if want_row:
            acc[row_slot, :, rows] += dot(vt[col_slot, :, cols], kern, NT)

    def own_part(row_slot, rep_slot):
        def one(u, _):
            half, j = u // N_CHUNK, u % N_CHUNK
            start = half * ROWS
            rows = pl.ds(pl.multiple_of(start, ROWS), ROWS)
            cols = rows_of(j)
            gram = dot(xs[row_slot, rows, :], xs[OWN, cols, :], NT)
            shift = arep[rep_slot, rows, :]
            shift = jnp.concatenate([shift, shift], axis=1)
            expo = jnp.minimum(gram * two_coef - shift - nrm[OWN, :, cols] * coef_2, top_2)
            kern = jnp.exp2(expo).astype(jnp.bfloat16)
            acc[OWN, :, cols] += dot(vt[row_slot, :, rows], kern, NN)
            return 0
        lax.fori_loop(0, 2 * N_CHUNK, one, 0)

    own_part(OWN, R_OWN)
    for c in (C_M1, C_P1, C_T0):
        n_copy(c).start()
    v_copy(C_T0).wait_recv()
    n_copy(C_T0).wait_recv()
    t0_copy().wait_recv()
    column_norms(T0, R_T0, 0, n_rows)
    v_copy(C_M1).wait_recv()
    n_copy(C_M1).wait_recv()
    v_copy(C_P1).wait_recv()
    n_copy(C_P1).wait_recv()
    for c in (C_M2, C_P2, C_T1):
        v_copy(c).start()
        n_copy(c).start()
    own_part(T0, R_T0)
    column_norms(M1, R_M1, 0, n_rows)
    column_norms(P1, R_P1, 0, n_rows)
    v_copy(C_T1).wait_recv()
    n_copy(C_T1).wait_recv()
    column_norms(T1, R_T1, 0, n_rows)

    def near_step(j, _):
        k = flip(j)
        x_copy(C_P1, k).wait_recv()
        x_copy(C_T1, k).start()
        x_copy(C_P2, k).start()
        x_copy(C_M1, j).wait_recv()
        x_copy(C_M2, j).start()

        x_copy(C_T1, k).wait_recv()

        def one(h, _):
            unit(OWN, h * ROWS, R_OWN, h * ROWS, P1, k, True)
            unit(OWN, h * ROWS, R_OWN, h * ROWS, T1, k, True)
            return 0
        lax.fori_loop(0, 2, one, 0)

        lo = jnp.where(j < 3, 4, jnp.where(j == 3, 0, j))
        hi = jnp.where(j < 3, 4, j + 1)

        def two(i, _):
            unit(M1, 0, R_M1, 0, P1, flip(i), True)
            unit(M1, 0, R_M1, 0, T1, flip(i), True)
            return 0
        lax.fori_loop(lo, hi, two, 0)
        return 0

    lax.fori_loop(0, N_CHUNK, near_step, 0)

    def rest(i, _):
        unit(M1, ROWS, R_M1, ROWS, P1, i, True)
        unit(M1, ROWS, R_M1, ROWS, T1, i, True)
        return 0
    lax.fori_loop(0, N_CHUNK, rest, 0)

    v_copy(C_M2).wait_recv()
    n_copy(C_M2).wait_recv()
    v_copy(C_P2).wait_recv()
    n_copy(C_P2).wait_recv()
    v_copy(C_TF).start()
    n_copy(C_TF).start()
    column_norms(far_row, R_FAR, far_base, ROWS)
    v_copy(C_TF).wait_recv()
    n_copy(C_TF).wait_recv()

    def far_step(j, _):
        k = flip(j)
        m = jnp.where(far_half == 0, k, j)
        x_copy(C_M2, j).wait_recv()
        x_copy(C_P2, k).wait_recv()
        x_copy(C_TF, m).start()

        def one(h, _):
            unit(P1, h * ROWS, R_P1, h * ROWS, M2, j, True)
            unit(T1, h * ROWS, R_T1, h * ROWS, M2, j, True)
            return 0
        lax.fori_loop(0, 2, one, 0)
        x_copy(C_TF, m).wait_recv()

        lo = jnp.where(j < 3, 4, jnp.where(j == 3, 0, j))
        hi = jnp.where(j < 3, 4, j + 1)

        def two(i, _):
            q = jnp.where(far_half == 0, flip(i), i)
            unit(far_row, far_base, R_FAR, 0, far_col, q, True)
            unit_far(q)
            return 0

        def unit_far(q):
            rows = pl.ds(far_base, ROWS)
            cols = rows_of(q)
            gram = dot(xs[far_row, rows, :], xs[TF, cols, :], NT)
            shift = arep[R_FAR, 0:ROWS, :]
            shift = jnp.concatenate([shift, shift], axis=1)
            expo = jnp.minimum(gram * two_coef - shift - nrm[TF, :, cols] * coef_2, top_2)
            kern = jnp.exp2(expo).astype(jnp.bfloat16)
            acc[TF, :, cols] += dot(vt[far_row, :, rows], kern, NN)
            acc[far_row, :, rows] += dot(vt[TF, :, cols], kern, NT)
        lax.fori_loop(lo, hi, two, 0)
        return 0

    lax.fori_loop(0, N_CHUNK, far_step, 0)

    r_copy(T1, 0, partner).start()
    r_copy(TF, 1, partner).start()
    r_copy(TF, 1, partner).wait_recv()
    acc[far_col] += rx[1]
    r_copy(M2, 2, down).start()
    r_copy(P2, 3, up).start()
    r_copy(T1, 0, partner).wait_recv()
    acc[P1] += rx[0]
    r_copy(M2, 2, down).wait_recv()
    acc[M1] += rx[2]
    r_copy(M1, 4, down).start()
    r_copy(P2, 3, up).wait_recv()
    acc[P1] += rx[3]
    r_copy(P1, 5, up).start()
    r_copy(M1, 4, down).wait_recv()
    r_copy(P1, 5, up).wait_recv()
    y_ref[...] = acc[OWN] + rx[4] + rx[5]

    def drain(j, _):
        for c in (C_M1, C_P1, C_M2, C_P2, C_T1, C_TF):
            x_copy(c, j).wait_send()
        return 0
    lax.fori_loop(0, N_CHUNK, drain, 0)
    t0_copy().wait_send()
    for c in range(7):
        v_copy(c).wait_send()
        n_copy(c).wait_send()
    for i, (src, to) in enumerate(((T1, partner), (TF, partner), (M2, down), (P2, up), (M1, down), (P1, up))):
        r_copy(src, i, to).wait_send()


def solution(mesh):
    n_group = mesh.shape['group']
    row_spec = P(('tasks', 'group'), None)

    def local_fn(x_loc, v_loc, lengthscale, outscale):
        n_rows, n_feat = x_loc.shape
        n_rhs = v_loc.shape[1]
        smem = pl.BlockSpec(memory_space=pltpu.SMEM)
        vmem = pl.BlockSpec(memory_space=pltpu.VMEM)

        def body(*refs):
            kernel(n_group, *refs)

        y_t = pl.pallas_call(
            body,
            name='gauss_ring',
            out_shape=jax.ShapeDtypeStruct((n_rhs, n_rows), jnp.float32),
            in_specs=[smem, smem, pl.BlockSpec(memory_space=pl.ANY), vmem],
            out_specs=vmem,
            scratch_shapes=[
                pltpu.VMEM((8, n_rows, n_feat), jnp.bfloat16),
                pltpu.VMEM((8, n_rhs, n_rows), jnp.bfloat16),
                pltpu.VMEM((8, 1, n_rows), jnp.float32),
                pltpu.VMEM((6, n_rows, 128), jnp.float32),
                pltpu.VMEM((8, n_rhs, n_rows), jnp.float32),
                pltpu.VMEM((6, n_rhs, n_rows), jnp.float32),
                pltpu.SemaphoreType.DMA((N_CHUNK,)),
                pltpu.SemaphoreType.DMA((6, N_CHUNK)),
                pltpu.SemaphoreType.DMA((6, N_CHUNK)),
                pltpu.SemaphoreType.DMA((7,)),
                pltpu.SemaphoreType.DMA((7,)),
                pltpu.SemaphoreType.DMA((7,)),
                pltpu.SemaphoreType.DMA((7,)),
                pltpu.SemaphoreType.DMA((2,)),
                pltpu.SemaphoreType.DMA((6,)),
                pltpu.SemaphoreType.DMA((6,)),
            ],
            compiler_params=pltpu.CompilerParams(
                collective_id=0, has_side_effects=True, vmem_limit_bytes=56 * 2**20),
        )(lengthscale, outscale, x_loc, v_loc.T)
        return y_t.T

    return jax.shard_map(local_fn, mesh=mesh, in_specs=(row_spec, row_spec, P(None), P(None)), out_specs=row_spec, check_vma=False)
```

```python
import jax
import jax.numpy as jnp
from jax import lax
from jax.experimental import pallas as pl
from jax.experimental.pallas import tpu as pltpu
from jax.sharding import PartitionSpec as P

MESH = pl.DeviceIdType.MESH
LOG2E = 1.4426950408889634
M2, M1, OWN, P1, P2, T0, T1, T2, TM2 = range(9)
N_SLOT = 9
R_OWN, R_T0, R_P1, R_T1, R_P2, R_T2, R_FAR, R_TFAR = range(8)
N_REP = 8
NT = (((1,), (1,)), ((), ()))
NN = (((1,), (0,)), ((), ()))
C_M1, C_P1, C_M2, C_P2, C_T1, C_T2, C_TM2, C_T0 = range(8)
N_CHUNK = 8
TILE = 256


def dot(a, b, dims):
    return lax.dot_general(a, b, dims, preferred_element_type=jnp.float32)


def kernel(n_group, ell_ref, s_ref, x_ref, v_ref, y_ref, xs, vt, nrm, arep, acc, rx,
           load_sem, x_send, x_recv, v_send, v_recv, n_send, n_recv, t0_sem, r_send, r_recv):
    n_rows = x_ref.shape[0]
    n_chip = n_group // 2
    me = lax.axis_index('group')
    chip, core = me // 2, me % 2
    up = ((chip + 1) % n_chip) * 2 + core
    down = ((chip + n_chip - 1) % n_chip) * 2 + core
    partner = chip * 2 + 1 - core
    far = chip // (n_chip // 2)
    far_w = M2 + (P2 - M2) * far
    far_l = P2 - (P2 - M2) * far
    far_t = T2 + (TM2 - T2) * far

    def rows_of(j):
        return pl.ds(pl.multiple_of(j * TILE, TILE), TILE)

    def flip(j):
        return (j + N_CHUNK // 2) % N_CHUNK

    SRC = {C_M1: OWN, C_P1: OWN, C_M2: M1, C_P2: P1, C_T1: P1, C_T2: P2, C_TM2: M2, C_T0: OWN}
    DST = {C_M1: M1, C_P1: P1, C_M2: M2, C_P2: P2, C_T1: T1, C_T2: T2, C_TM2: TM2, C_T0: T0}
    TO = {C_M1: up, C_P1: down, C_M2: up, C_P2: down, C_T1: partner, C_T2: partner, C_TM2: partner, C_T0: partner}

    def x_copy(c, j):
        return pltpu.make_async_remote_copy(
            src_ref=xs.at[SRC[c], rows_of(j)], dst_ref=xs.at[DST[c], rows_of(j)],
            send_sem=x_send.at[c, j], recv_sem=x_recv.at[c, j],
            device_id={'group': TO[c]}, device_id_type=MESH)

    def t0_copy():
        return pltpu.make_async_remote_copy(
            src_ref=xs.at[OWN], dst_ref=xs.at[T0], send_sem=t0_sem.at[0], recv_sem=t0_sem.at[1],
            device_id={'group': partner}, device_id_type=MESH)

    def v_copy(c):
        src = v_ref if c in (C_M1, C_P1, C_T0) else vt.at[SRC[c]]
        return pltpu.make_async_remote_copy(
            src_ref=src, dst_ref=vt.at[DST[c]], send_sem=v_send.at[c], recv_sem=v_recv.at[c],
            device_id={'group': TO[c]}, device_id_type=MESH)

    def n_copy(c):
        return pltpu.make_async_remote_copy(
            src_ref=nrm.at[SRC[c]], dst_ref=nrm.at[DST[c]], send_sem=n_send.at[c], recv_sem=n_recv.at[c],
            device_id={'group': TO[c]}, device_id_type=MESH)

    def r_copy(src, i, to):
        return pltpu.make_async_remote_copy(
            src_ref=acc.at[src], dst_ref=rx.at[i], send_sem=r_send.at[i], recv_sem=r_recv.at[i],
            device_id={'group': to}, device_id_type=MESH)

    def load(j):
        return pltpu.make_async_copy(x_ref.at[rows_of(j)], xs.at[OWN, rows_of(j)], load_sem.at[j])

    for j in range(N_CHUNK):
        load(j).start()
    barrier = pltpu.get_barrier_semaphore()
    for peer in (up, down, partner):
        pl.semaphore_signal(barrier, inc=1, device_id={'group': peer}, device_id_type=MESH)
    pl.semaphore_wait(barrier, 3)
    for c in (C_M1, C_P1, C_T0):
        v_copy(c).start()
    for j in range(N_CHUNK):
        load(j).wait()
    for j in range(N_CHUNK):
        x_copy(C_M1, j).start()
        x_copy(C_P1, flip(j)).start()
    t0_copy().start()

    ell = jnp.full((1, 128), ell_ref[0], jnp.float32)
    coef = LOG2E / (2.0 * jnp.square(ell))
    top = LOG2E * jnp.log(jnp.full((1, 128), s_ref[0], jnp.float32))

    acc[...] = jnp.zeros_like(acc)
    vt[OWN] = v_ref[...]

    def own_norms(b, _):
        rows = pl.ds(pl.multiple_of(b * 128, 128), 128)
        part = jnp.sum(jnp.square(xs[OWN, rows, :].astype(jnp.float32)), axis=1, keepdims=True)
        part = jnp.broadcast_to(part, (128, 128))
        arep[R_OWN, rows, :] = part * coef - top
        nrm[OWN, :, rows] = part.T[0:1, :]
        return 0

    lax.fori_loop(0, n_rows // 128, own_norms, 0)

    def column_norms(slot, rep):
        def one(b, _):
            rows = pl.ds(pl.multiple_of(b * 128, 128), 128)
            row = jnp.broadcast_to(nrm[slot, :, rows], (128, 128))
            arep[rep, rows, :] = row.T * coef - top
            return 0
        lax.fori_loop(0, n_rows // 128, one, 0)

    def wide(v, n):
        return jnp.concatenate([v] * (n // 128), axis=1)

    def kern_of(left, shift, w, cols, n):
        gram = dot(left, xs[w, cols, :], NT)
        expo = gram * wide(2.0 * coef, n) - wide(shift, n) - nrm[w, :, cols] * wide(coef, n)
        return jnp.exp2(jnp.minimum(expo, wide(top, n))).astype(jnp.bfloat16)

    def pair(la, ja, ra, lb, jb, rb, w, base, n, sides=True, yw=None):
        cols = pl.ds(pl.multiple_of(base, TILE), n)
        a, b = rows_of(ja), rows_of(jb)
        left = jnp.concatenate([xs[la, a, :], xs[lb, b, :]], axis=0)
        shift = jnp.concatenate([arep[ra, a, :], arep[rb, b, :]], axis=0)
        kern = kern_of(left, shift, w, cols, n)
        v = jnp.concatenate([vt[la, :, a], vt[lb, :, b]], axis=1)
        acc[w, :, cols] += dot(v, kern, NN)
        if sides:
            y = dot(vt[w, :, cols], kern, NT)
            acc[la, :, a] += y[:, :TILE]
            acc[lb, :, b] += y[:, TILE:]

    def single(la, ja, ra, w):
        a = rows_of(ja)
        kern = kern_of(xs[la, a, :], arep[ra, a, :], w, slice(None), n_rows)
        acc[w] += dot(vt[la, :, a], kern, NN)
        acc[la, :, a] += dot(vt[w], kern, NT)

    def own_pairs(slot, rep):
        def one(i, _):
            pair(slot, 2 * i, rep, slot, 2 * i + 1, rep, OWN, 0, n_rows, sides=False)
            return 0
        lax.fori_loop(0, N_CHUNK // 2, one, 0)

    own_pairs(OWN, R_OWN)
    for c in (C_M1, C_P1, C_T0):
        n_copy(c).start()
    v_copy(C_T0).wait_recv()
    n_copy(C_T0).wait_recv()
    t0_copy().wait_recv()
    column_norms(T0, R_T0)
    v_copy(C_M1).wait_recv()
    n_copy(C_M1).wait_recv()
    v_copy(C_P1).wait_recv()
    n_copy(C_P1).wait_recv()
    for c in (C_M2, C_P2, C_T1):
        v_copy(c).start()
        n_copy(c).start()
    own_pairs(T0, R_T0)
    column_norms(P1, R_P1)
    v_copy(C_T1).wait_recv()
    n_copy(C_T1).wait_recv()
    column_norms(T1, R_T1)

    def mid(i, start):
        k = flip(i)
        pair(P1, k, R_P1, T1, k, R_T1, M1, start, n_rows // 2)

    def near_step(j, _):
        @pl.when(j < N_CHUNK)
        def _():
            k = flip(j)
            x_copy(C_P1, k).wait_recv()
            x_copy(C_T1, k).start()
            x_copy(C_P2, k).start()
            x_copy(C_M1, j).wait_recv()
            x_copy(C_M2, j).start()

        @pl.when(j > 0)
        def _():
            i = j - 1
            k = flip(i)
            x_copy(C_T1, k).wait_recv()
            pair(P1, k, R_P1, T1, k, R_T1, OWN, 0, n_rows)

            def one(i, _):
                mid(i, 0)
                return 0
            lax.fori_loop(jnp.where(j < 4, N_CHUNK, jnp.where(j == 4, 0, i)), jnp.where(j < 4, N_CHUNK, j), one, 0)
        return 0

    lax.fori_loop(0, N_CHUNK + 1, near_step, 0)

    for c in (C_M2, C_P2):
        v_copy(c).wait_recv()
        n_copy(c).wait_recv()
    for c in (C_T2, C_TM2):
        v_copy(c).start()
        n_copy(c).start()
    column_norms(P2, R_P2)
    mid(N_CHUNK - 1, n_rows // 2)
    for c in (C_T2, C_TM2):
        v_copy(c).wait_recv()
        n_copy(c).wait_recv()
    column_norms(T2, R_T2)
    column_norms(far_l, R_FAR)
    column_norms(far_t, R_TFAR)

    def arrive(j):
        k = flip(j)
        x_copy(C_P2, k).wait_recv()
        x_copy(C_T2, k).start()
        x_copy(C_M2, j).wait_recv()
        x_copy(C_TM2, j).start()

    def far_pair(i):
        q = jnp.where(far == 0, flip(i), i)
        pair(far_l, q, R_FAR, far_t, q, R_TFAR, far_w, far * (n_rows // 2), n_rows // 2)

    def far_step(j, _):
        k = flip(j)
        arrive(j)
        mid(j, n_rows // 2)
        x_copy(C_T2, k).wait_recv()
        x_copy(C_TM2, j).wait_recv()
        pair(P2, k, R_P2, T2, k, R_T2, M1, 0, n_rows)

        def one(i, _):
            far_pair(i)
            return 0
        lax.fori_loop(jnp.where(j < 3, N_CHUNK, jnp.where(j == 3, 0, j)), jnp.where(j < 3, N_CHUNK, j + 1), one, 0)
        return 0

    lax.fori_loop(0, N_CHUNK - 1, far_step, 0)

    ways = ((T1, partner), (T2, partner), (TM2, partner), (M2, down), (P2, up), (M1, down), (P1, up))

    def back(i):
        return r_copy(ways[i][0], i, ways[i][1])

    back(0).start()
    final = N_CHUNK - 1
    arrive(final)
    single(P2, flip(final), R_P2, M1)
    x_copy(C_T2, flip(final)).wait_recv()
    single(T2, flip(final), R_T2, M1)
    x_copy(C_TM2, final).wait_recv()
    far_pair(final)
    back(2).start()
    back(1).start()
    back(2).wait_recv()
    acc[M2] += rx[2]
    back(3).start()
    back(1).wait_recv()
    acc[P2] += rx[1]
    back(4).start()
    back(0).wait_recv()
    acc[P1] += rx[0]
    back(3).wait_recv()
    acc[M1] += rx[3]
    back(5).start()
    back(4).wait_recv()
    acc[P1] += rx[4]
    back(6).start()
    back(5).wait_recv()
    back(6).wait_recv()
    y_ref[...] = acc[OWN] + rx[5] + rx[6]

    def drain(j, _):
        for c in (C_M1, C_P1, C_M2, C_P2, C_T1, C_T2, C_TM2):
            x_copy(c, j).wait_send()
        return 0
    lax.fori_loop(0, N_CHUNK, drain, 0)
    t0_copy().wait_send()
    for c in range(8):
        v_copy(c).wait_send()
        n_copy(c).wait_send()
    for i in range(len(ways)):
        back(i).wait_send()


def solution(mesh):
    n_group = mesh.shape['group']
    row_spec = P(('tasks', 'group'), None)

    def local_fn(x_loc, v_loc, lengthscale, outscale):
        n_rows, n_feat = x_loc.shape
        n_rhs = v_loc.shape[1]
        smem = pl.BlockSpec(memory_space=pltpu.SMEM)
        vmem = pl.BlockSpec(memory_space=pltpu.VMEM)

        def body(*refs):
            kernel(n_group, *refs)

        y_t = pl.pallas_call(
            body,
            name='gauss_ring',
            out_shape=jax.ShapeDtypeStruct((n_rhs, n_rows), jnp.float32),
            in_specs=[smem, smem, pl.BlockSpec(memory_space=pl.ANY), vmem],
            out_specs=vmem,
            scratch_shapes=[
                pltpu.VMEM((N_SLOT, n_rows, n_feat), jnp.bfloat16),
                pltpu.VMEM((N_SLOT, n_rhs, n_rows), jnp.bfloat16),
                pltpu.VMEM((N_SLOT, 1, n_rows), jnp.float32),
                pltpu.VMEM((N_REP, n_rows, 128), jnp.float32),
                pltpu.VMEM((N_SLOT, n_rhs, n_rows), jnp.float32),
                pltpu.VMEM((7, n_rhs, n_rows), jnp.float32),
                pltpu.SemaphoreType.DMA((N_CHUNK,)),
                pltpu.SemaphoreType.DMA((7, N_CHUNK)),
                pltpu.SemaphoreType.DMA((7, N_CHUNK)),
                pltpu.SemaphoreType.DMA((8,)),
                pltpu.SemaphoreType.DMA((8,)),
                pltpu.SemaphoreType.DMA((8,)),
                pltpu.SemaphoreType.DMA((8,)),
                pltpu.SemaphoreType.DMA((2,)),
                pltpu.SemaphoreType.DMA((7,)),
                pltpu.SemaphoreType.DMA((7,)),
            ],
            compiler_params=pltpu.CompilerParams(
                collective_id=0, has_side_effects=True, vmem_limit_bytes=58 * 2**20),
        )(lengthscale, outscale, x_loc, v_loc.T)
        return y_t.T

    return jax.shard_map(local_fn, mesh=mesh, in_specs=(row_spec, row_spec, P(None), P(None)), out_specs=row_spec, check_vma=False)
```

```python
import jax
import jax.numpy as jnp
from jax import lax
from jax.experimental import pallas as pl
from jax.experimental.pallas import tpu as pltpu
from jax.sharding import PartitionSpec as P

MESH = pl.DeviceIdType.MESH
LOG2E = 1.4426950408889634
M2, M1, OWN, P1, P2, T0, T1, T2, TM2 = range(9)
N_SLOT = 9
R_OWN, R_T0, R_P1, R_T1, R_P2, R_T2, R_FAR, R_TFAR = range(8)
N_REP = 8
NT = (((1,), (1,)), ((), ()))
NN = (((1,), (0,)), ((), ()))
C_M1, C_P1, C_M2, C_P2, C_T1, C_T2, C_TM2, C_T0 = range(8)
N_CHUNK = 8
TILE = 256


def dot(a, b, dims):
    return lax.dot_general(a, b, dims, preferred_element_type=jnp.float32)


def kernel(n_group, ell_ref, s_ref, x_ref, v_ref, y_ref, xs, vt, nrm, arep, acc, rx,
           load_sem, x_send, x_recv, v_send, v_recv, n_send, n_recv, t0_sem, r_send, r_recv):
    n_rows = x_ref.shape[0]
    n_chip = n_group // 2
    me = lax.axis_index('group')
    chip, core = me // 2, me % 2
    up = ((chip + 1) % n_chip) * 2 + core
    down = ((chip + n_chip - 1) % n_chip) * 2 + core
    partner = chip * 2 + 1 - core
    far = chip // (n_chip // 2)
    far_w = M2 + (P2 - M2) * far
    far_l = P2 - (P2 - M2) * far
    far_t = T2 + (TM2 - T2) * far

    def rows_of(j):
        return pl.ds(pl.multiple_of(j * TILE, TILE), TILE)

    def flip(j):
        return (j + N_CHUNK // 2) % N_CHUNK

    SRC = {C_M1: OWN, C_P1: OWN, C_M2: M1, C_P2: P1, C_T1: P1, C_T2: P2, C_TM2: M2, C_T0: OWN}
    DST = {C_M1: M1, C_P1: P1, C_M2: M2, C_P2: P2, C_T1: T1, C_T2: T2, C_TM2: TM2, C_T0: T0}
    TO = {C_M1: up, C_P1: down, C_M2: up, C_P2: down, C_T1: partner, C_T2: partner, C_TM2: partner, C_T0: partner}

    def x_copy(c, j):
        return pltpu.make_async_remote_copy(
            src_ref=xs.at[SRC[c], rows_of(j)], dst_ref=xs.at[DST[c], rows_of(j)],
            send_sem=x_send.at[c, j], recv_sem=x_recv.at[c, j],
            device_id={'group': TO[c]}, device_id_type=MESH)

    def t0_copy():
        return pltpu.make_async_remote_copy(
            src_ref=xs.at[OWN], dst_ref=xs.at[T0], send_sem=t0_sem.at[0], recv_sem=t0_sem.at[1],
            device_id={'group': partner}, device_id_type=MESH)

    def v_copy(c):
        src = v_ref if c in (C_M1, C_P1, C_T0) else vt.at[SRC[c]]
        return pltpu.make_async_remote_copy(
            src_ref=src, dst_ref=vt.at[DST[c]], send_sem=v_send.at[c], recv_sem=v_recv.at[c],
            device_id={'group': TO[c]}, device_id_type=MESH)

    def n_copy(c):
        return pltpu.make_async_remote_copy(
            src_ref=nrm.at[SRC[c]], dst_ref=nrm.at[DST[c]], send_sem=n_send.at[c], recv_sem=n_recv.at[c],
            device_id={'group': TO[c]}, device_id_type=MESH)

    def r_copy(src, i, to):
        return pltpu.make_async_remote_copy(
            src_ref=acc.at[src], dst_ref=rx.at[i], send_sem=r_send.at[i], recv_sem=r_recv.at[i],
            device_id={'group': to}, device_id_type=MESH)

    def load(j):
        return pltpu.make_async_copy(x_ref.at[rows_of(j)], xs.at[OWN, rows_of(j)], load_sem.at[j])

    for j in range(N_CHUNK):
        load(j).start()
    barrier = pltpu.get_barrier_semaphore()
    for peer in (up, down, partner):
        pl.semaphore_signal(barrier, inc=1, device_id={'group': peer}, device_id_type=MESH)
    pl.semaphore_wait(barrier, 3)
    for c in (C_M1, C_P1, C_T0):
        v_copy(c).start()
    for j in range(N_CHUNK):
        load(j).wait()

    def send_own(first, last):
        for j in range(first, last):
            x_copy(C_M1, j).start()
            x_copy(C_P1, flip(j)).start()

    send_own(0, 1)
    t0_copy().start()

    ell = jnp.full((1, 128), ell_ref[0], jnp.float32)
    coef = LOG2E / (2.0 * jnp.square(ell))
    top = LOG2E * jnp.log(jnp.full((1, 128), s_ref[0], jnp.float32))

    acc[...] = jnp.zeros_like(acc)
    vt[OWN] = v_ref[...]

    for b in range(n_rows // 128):
        rows = slice(b * 128, (b + 1) * 128)
        part = jnp.sum(jnp.square(xs[OWN, rows, :].astype(jnp.float32)), axis=1, keepdims=True)
        part = jnp.broadcast_to(part, (128, 128))
        arep[R_OWN, rows, :] = part * coef - top
        nrm[OWN, :, rows] = part.T[0:1, :]
    for c in (C_M1, C_P1, C_T0):
        n_copy(c).start()
    send_own(1, N_CHUNK // 2)

    def column_norms(slot, rep):
        for b in range(n_rows // 128):
            rows = slice(b * 128, (b + 1) * 128)
            row = jnp.broadcast_to(nrm[slot, :, rows], (128, 128))
            arep[rep, rows, :] = row.T * coef - top

    def wide(v, n):
        return jnp.concatenate([v] * (n // 128), axis=1)

    def kern_of(left, shift, w, cols, n):
        gram = dot(left, xs[w, cols, :], NT)
        expo = gram * wide(2.0 * coef, n) - wide(shift, n) - nrm[w, :, cols] * wide(coef, n)
        return jnp.exp2(jnp.minimum(expo, wide(top, n))).astype(jnp.bfloat16)

    def pair(la, ja, ra, lb, jb, rb, w, base, n, sides=True, yw=None):
        cols = pl.ds(pl.multiple_of(base, TILE), n)
        a, b = rows_of(ja), rows_of(jb)
        left = jnp.concatenate([xs[la, a, :], xs[lb, b, :]], axis=0)
        shift = jnp.concatenate([arep[ra, a, :], arep[rb, b, :]], axis=0)
        kern = kern_of(left, shift, w, cols, n)
        v = jnp.concatenate([vt[la, :, a], vt[lb, :, b]], axis=1)
        acc[w, :, cols] += dot(v, kern, NN)
        if sides:
            y = dot(vt[w, :, cols], kern, NT)
            acc[la, :, a] += y[:, :TILE]
            acc[lb, :, b] += y[:, TILE:]

    def single(la, ja, ra, w):
        a = rows_of(ja)
        kern = kern_of(xs[la, a, :], arep[ra, a, :], w, slice(None), n_rows)
        acc[w] += dot(vt[la, :, a], kern, NN)
        acc[la, :, a] += dot(vt[w], kern, NT)

    def own_pairs(slot, rep):
        def one(i, _):
            pair(slot, 2 * i, rep, slot, 2 * i + 1, rep, OWN, 0, n_rows, sides=False)
            return 0
        lax.fori_loop(0, N_CHUNK // 2, one, 0)

    own_pairs(OWN, R_OWN)
    v_copy(C_T0).wait_recv()
    n_copy(C_T0).wait_recv()
    t0_copy().wait_recv()
    column_norms(T0, R_T0)
    own_pairs(T0, R_T0)
    for c in (C_M1, C_P1):
        v_copy(c).wait_recv()
        n_copy(c).wait_recv()
    for c in (C_M2, C_P2, C_T1):
        v_copy(c).start()
        n_copy(c).start()
    send_own(N_CHUNK // 2, N_CHUNK)
    column_norms(P1, R_P1)
    v_copy(C_T1).wait_recv()
    n_copy(C_T1).wait_recv()
    column_norms(T1, R_T1)

    def mid(i, start):
        k = flip(i)
        pair(P1, k, R_P1, T1, k, R_T1, M1, start, n_rows // 2)

    def near_step(j, _):
        @pl.when(j < N_CHUNK)
        def _():
            k = flip(j)
            x_copy(C_P1, k).wait_recv()
            x_copy(C_T1, k).start()
            x_copy(C_P2, k).start()
            x_copy(C_M1, j).wait_recv()
            x_copy(C_M2, j).start()

        @pl.when(j > 0)
        def _():
            i = j - 1
            k = flip(i)
            x_copy(C_T1, k).wait_recv()
            pair(P1, k, R_P1, T1, k, R_T1, OWN, 0, n_rows)

            def one(i, _):
                mid(i, 0)
                return 0
            lax.fori_loop(jnp.where(j < 4, N_CHUNK, jnp.where(j == 4, 0, i)), jnp.where(j < 4, N_CHUNK, j), one, 0)
        return 0

    lax.fori_loop(0, N_CHUNK - 2, near_step, 0)
    for c in (C_M2, C_P2):
        v_copy(c).wait_recv()
        n_copy(c).wait_recv()
    for c in (C_T2, C_TM2):
        v_copy(c).start()
        n_copy(c).start()
    column_norms(P2, R_P2)
    for c in (C_T2, C_TM2):
        v_copy(c).wait_recv()
        n_copy(c).wait_recv()
    column_norms(T2, R_T2)
    column_norms(far_l, R_FAR)
    column_norms(far_t, R_TFAR)
    lax.fori_loop(N_CHUNK - 2, N_CHUNK + 1, near_step, 0)

    mid(N_CHUNK - 1, n_rows // 2)

    def arrive(j):
        k = flip(j)
        x_copy(C_P2, k).wait_recv()
        x_copy(C_T2, k).start()
        x_copy(C_M2, j).wait_recv()
        x_copy(C_TM2, j).start()

    def far_pair(i):
        q = jnp.where(far == 0, flip(i), i)
        pair(far_l, q, R_FAR, far_t, q, R_TFAR, far_w, far * (n_rows // 2), n_rows // 2)

    def far_step(j, _):
        k = flip(j)
        arrive(j)
        mid(j, n_rows // 2)
        x_copy(C_T2, k).wait_recv()
        x_copy(C_TM2, j).wait_recv()
        pair(P2, k, R_P2, T2, k, R_T2, M1, 0, n_rows)

        def one(i, _):
            far_pair(i)
            return 0
        lax.fori_loop(jnp.where(j < 3, N_CHUNK, jnp.where(j == 3, 0, j)), jnp.where(j < 3, N_CHUNK, j + 1), one, 0)
        return 0

    lax.fori_loop(0, N_CHUNK - 1, far_step, 0)

    ways = ((T1, partner), (T2, partner), (TM2, partner), (M2, down), (P2, up), (M1, down), (P1, up))

    def back(i):
        return r_copy(ways[i][0], i, ways[i][1])

    back(0).start()
    final = N_CHUNK - 1
    arrive(final)
    single(P2, flip(final), R_P2, M1)
    x_copy(C_T2, flip(final)).wait_recv()
    single(T2, flip(final), R_T2, M1)
    x_copy(C_TM2, final).wait_recv()
    far_pair(final)
    back(2).start()
    back(1).start()
    back(2).wait_recv()
    acc[M2] += rx[2]
    back(3).start()
    back(1).wait_recv()
    acc[P2] += rx[1]
    back(4).start()
    back(0).wait_recv()
    acc[P1] += rx[0]
    back(3).wait_recv()
    acc[M1] += rx[3]
    back(5).start()
    back(4).wait_recv()
    acc[P1] += rx[4]
    back(6).start()
    back(5).wait_recv()
    back(6).wait_recv()
    y_ref[...] = acc[OWN] + rx[5] + rx[6]

    def drain(j, _):
        for c in (C_M1, C_P1, C_M2, C_P2, C_T1, C_T2, C_TM2):
            x_copy(c, j).wait_send()
        return 0
    lax.fori_loop(0, N_CHUNK, drain, 0)
    t0_copy().wait_send()
    for c in range(8):
        v_copy(c).wait_send()
        n_copy(c).wait_send()
    for i in range(len(ways)):
        back(i).wait_send()


def solution(mesh):
    n_group = mesh.shape['group']
    row_spec = P(('tasks', 'group'), None)

    def local_fn(x_loc, v_loc, lengthscale, outscale):
        n_rows, n_feat = x_loc.shape
        n_rhs = v_loc.shape[1]
        smem = pl.BlockSpec(memory_space=pltpu.SMEM)
        vmem = pl.BlockSpec(memory_space=pltpu.VMEM)

        def body(*refs):
            kernel(n_group, *refs)

        y_t = pl.pallas_call(
            body,
            name='gauss_ring',
            out_shape=jax.ShapeDtypeStruct((n_rhs, n_rows), jnp.float32),
            in_specs=[smem, smem, pl.BlockSpec(memory_space=pl.ANY), vmem],
            out_specs=vmem,
            scratch_shapes=[
                pltpu.VMEM((N_SLOT, n_rows, n_feat), jnp.bfloat16),
                pltpu.VMEM((N_SLOT, n_rhs, n_rows), jnp.bfloat16),
                pltpu.VMEM((N_SLOT, 1, n_rows), jnp.float32),
                pltpu.VMEM((N_REP, n_rows, 128), jnp.float32),
                pltpu.VMEM((N_SLOT, n_rhs, n_rows), jnp.float32),
                pltpu.VMEM((7, n_rhs, n_rows), jnp.float32),
                pltpu.SemaphoreType.DMA((N_CHUNK,)),
                pltpu.SemaphoreType.DMA((7, N_CHUNK)),
                pltpu.SemaphoreType.DMA((7, N_CHUNK)),
                pltpu.SemaphoreType.DMA((8,)),
                pltpu.SemaphoreType.DMA((8,)),
                pltpu.SemaphoreType.DMA((8,)),
                pltpu.SemaphoreType.DMA((8,)),
                pltpu.SemaphoreType.DMA((2,)),
                pltpu.SemaphoreType.DMA((7,)),
                pltpu.SemaphoreType.DMA((7,)),
            ],
            compiler_params=pltpu.CompilerParams(
                collective_id=0, has_side_effects=True, vmem_limit_bytes=58 * 2**20),
        )(lengthscale, outscale, x_loc, v_loc.T)
        return y_t.T

    return jax.shard_map(local_fn, mesh=mesh, in_specs=(row_spec, row_spec, P(None), P(None)), out_specs=row_spec, check_vma=False)
```

```python
import jax
import jax.numpy as jnp
from jax import lax
from jax.experimental import pallas as pl
from jax.experimental.pallas import tpu as pltpu
from jax.sharding import PartitionSpec as P

MESH = pl.DeviceIdType.MESH
LOG2E = 1.4426950408889634
M2, M1, OWN, P1, P2, T0, T1, T2, TM2 = range(9)
N_SLOT = 9
R_OWN, R_T0, R_P1, R_T1, R_P2, R_T2, R_FAR, R_TFAR = range(8)
N_REP = 8
NT = (((1,), (1,)), ((), ()))
NN = (((1,), (0,)), ((), ()))
C_M1, C_P1, C_M2, C_P2, C_T1, C_T2, C_TM2, C_T0 = range(8)
N_CHUNK = 8
TILE = 256
N_PIECE = 4


def dot(a, b, dims):
    return lax.dot_general(a, b, dims, preferred_element_type=jnp.float32)


def kernel(n_group, ell_ref, s_ref, x_ref, v_ref, y_ref, xs, vt, nrm, arep, acc, rx,
           load_sem, x_send, x_recv, v_send, v_recv, n_send, n_recv, t0_sem, r_send, r_recv):
    n_rows = x_ref.shape[0]
    n_chip = n_group // 2
    me = lax.axis_index('group')
    chip, core = me // 2, me % 2
    up = ((chip + 1) % n_chip) * 2 + core
    down = ((chip + n_chip - 1) % n_chip) * 2 + core
    partner = chip * 2 + 1 - core
    far = chip // (n_chip // 2)
    far_w = M2 + (P2 - M2) * far
    far_l = P2 - (P2 - M2) * far
    far_t = T2 + (TM2 - T2) * far

    def rows_of(j):
        return pl.ds(pl.multiple_of(j * TILE, TILE), TILE)

    def flip(j):
        return (j + N_CHUNK // 2) % N_CHUNK

    SRC = {C_M1: OWN, C_P1: OWN, C_M2: M1, C_P2: P1, C_T1: P1, C_T2: P2, C_TM2: M2, C_T0: OWN}
    DST = {C_M1: M1, C_P1: P1, C_M2: M2, C_P2: P2, C_T1: T1, C_T2: T2, C_TM2: TM2, C_T0: T0}
    TO = {C_M1: up, C_P1: down, C_M2: up, C_P2: down, C_T1: partner, C_T2: partner, C_TM2: partner, C_T0: partner}

    def x_copy(c, j):
        return pltpu.make_async_remote_copy(
            src_ref=xs.at[SRC[c], rows_of(j)], dst_ref=xs.at[DST[c], rows_of(j)],
            send_sem=x_send.at[c, j], recv_sem=x_recv.at[c, j],
            device_id={'group': TO[c]}, device_id_type=MESH)

    def t0_copy():
        return pltpu.make_async_remote_copy(
            src_ref=xs.at[OWN], dst_ref=xs.at[T0], send_sem=t0_sem.at[0], recv_sem=t0_sem.at[1],
            device_id={'group': partner}, device_id_type=MESH)

    def v_copy(c):
        src = v_ref if c in (C_M1, C_P1, C_T0) else vt.at[SRC[c]]
        return pltpu.make_async_remote_copy(
            src_ref=src, dst_ref=vt.at[DST[c]], send_sem=v_send.at[c], recv_sem=v_recv.at[c],
            device_id={'group': TO[c]}, device_id_type=MESH)

    def n_copy(c):
        return pltpu.make_async_remote_copy(
            src_ref=nrm.at[SRC[c]], dst_ref=nrm.at[DST[c]], send_sem=n_send.at[c], recv_sem=n_recv.at[c],
            device_id={'group': TO[c]}, device_id_type=MESH)

    def piece(p):
        return slice(p * n_rows // N_PIECE, (p + 1) * n_rows // N_PIECE)

    def r_copy(src, i, to, p):
        return pltpu.make_async_remote_copy(
            src_ref=acc.at[src, :, piece(p)], dst_ref=rx.at[i, :, piece(p)],
            send_sem=r_send.at[i, p], recv_sem=r_recv.at[i, p],
            device_id={'group': to}, device_id_type=MESH)

    def load(j):
        return pltpu.make_async_copy(x_ref.at[rows_of(j)], xs.at[OWN, rows_of(j)], load_sem.at[j])

    order = [j for i in range(N_CHUNK // 2) for j in (i, flip(i))]
    for j in order:
        load(j).start()
    barrier = pltpu.get_barrier_semaphore()
    for peer in (up, down, partner):
        pl.semaphore_signal(barrier, inc=1, device_id={'group': peer}, device_id_type=MESH)
    pl.semaphore_wait(barrier, 3)
    for c in (C_M1, C_P1, C_T0):
        v_copy(c).start()
    def send_own(first, last):
        for j in range(first, last):
            x_copy(C_M1, j).start()
            x_copy(C_P1, flip(j)).start()

    for j in order[:2]:
        load(j).wait()
    send_own(0, 1)
    for j in order[2:]:
        load(j).wait()
    t0_copy().start()

    ell = jnp.full((1, 128), ell_ref[0], jnp.float32)
    coef = LOG2E / (2.0 * jnp.square(ell))
    top = LOG2E * jnp.log(jnp.full((1, 128), s_ref[0], jnp.float32))

    acc[...] = jnp.zeros_like(acc)
    vt[OWN] = v_ref[...]

    for b in range(n_rows // 128):
        rows = slice(b * 128, (b + 1) * 128)
        part = jnp.sum(jnp.square(xs[OWN, rows, :].astype(jnp.float32)), axis=1, keepdims=True)
        part = jnp.broadcast_to(part, (128, 128))
        arep[R_OWN, rows, :] = part * coef - top
        nrm[OWN, :, rows] = part.T[0:1, :]
    for c in (C_M1, C_P1, C_T0):
        n_copy(c).start()
    send_own(1, N_CHUNK // 2)

    def column_norms(slot, rep):
        for b in range(n_rows // 128):
            rows = slice(b * 128, (b + 1) * 128)
            row = jnp.broadcast_to(nrm[slot, :, rows], (128, 128))
            arep[rep, rows, :] = row.T * coef - top

    def wide(v, n):
        return jnp.concatenate([v] * (n // 128), axis=1)

    def kern_of(left, shift, w, cols, n):
        gram = dot(left, xs[w, cols, :], NT)
        expo = gram * wide(2.0 * coef, n) - wide(shift, n) - nrm[w, :, cols] * wide(coef, n)
        return jnp.exp2(jnp.minimum(expo, wide(top, n))).astype(jnp.bfloat16)

    def pair(la, ja, ra, lb, jb, rb, w, base, n, sides=True, yw=None):
        cols = pl.ds(pl.multiple_of(base, TILE), n)
        a, b = rows_of(ja), rows_of(jb)
        left = jnp.concatenate([xs[la, a, :], xs[lb, b, :]], axis=0)
        shift = jnp.concatenate([arep[ra, a, :], arep[rb, b, :]], axis=0)
        kern = kern_of(left, shift, w, cols, n)
        v = jnp.concatenate([vt[la, :, a], vt[lb, :, b]], axis=1)
        acc[w, :, cols] += dot(v, kern, NN)
        if sides:
            y = dot(vt[w, :, cols], kern, NT)
            acc[la, :, a] += y[:, :TILE]
            acc[lb, :, b] += y[:, TILE:]

    def own_pairs(slot, rep):
        def one(i, _):
            pair(slot, 2 * i, rep, slot, 2 * i + 1, rep, OWN, 0, n_rows, sides=False)
            return 0
        lax.fori_loop(0, N_CHUNK // 2, one, 0)

    own_pairs(OWN, R_OWN)
    v_copy(C_T0).wait_recv()
    n_copy(C_T0).wait_recv()
    t0_copy().wait_recv()
    column_norms(T0, R_T0)
    own_pairs(T0, R_T0)
    for c in (C_M1, C_P1):
        v_copy(c).wait_recv()
        n_copy(c).wait_recv()
    for c in (C_M2, C_P2, C_T1):
        v_copy(c).start()
        n_copy(c).start()
    send_own(N_CHUNK // 2, N_CHUNK)
    column_norms(P1, R_P1)
    v_copy(C_T1).wait_recv()
    n_copy(C_T1).wait_recv()
    column_norms(T1, R_T1)

    def mid(i, start):
        k = flip(i)
        pair(P1, k, R_P1, T1, k, R_T1, M1, start, n_rows // 2)

    def near_step(j, _):
        @pl.when(j < N_CHUNK)
        def _():
            k = flip(j)
            x_copy(C_P1, k).wait_recv()
            x_copy(C_T1, k).start()
            x_copy(C_P2, k).start()
            x_copy(C_M1, j).wait_recv()
            x_copy(C_M2, j).start()

        @pl.when(j > 0)
        def _():
            i = j - 1
            k = flip(i)
            x_copy(C_T1, k).wait_recv()
            pair(P1, k, R_P1, T1, k, R_T1, OWN, 0, n_rows)

            def one(i, _):
                mid(i, 0)
                return 0
            lax.fori_loop(jnp.where(j < 4, N_CHUNK, jnp.where(j == 4, 0, i)), jnp.where(j < 4, N_CHUNK, j), one, 0)
        return 0

    lax.fori_loop(0, N_CHUNK - 2, near_step, 0)
    for c in (C_M2, C_P2):
        v_copy(c).wait_recv()
        n_copy(c).wait_recv()
    for c in (C_T2, C_TM2):
        v_copy(c).start()
        n_copy(c).start()
    column_norms(P2, R_P2)
    for c in (C_T2, C_TM2):
        v_copy(c).wait_recv()
        n_copy(c).wait_recv()
    column_norms(T2, R_T2)
    column_norms(far_l, R_FAR)
    column_norms(far_t, R_TFAR)
    lax.fori_loop(N_CHUNK - 2, N_CHUNK + 1, near_step, 0)

    mid(N_CHUNK - 1, n_rows // 2)

    def arrive(j):
        k = flip(j)
        x_copy(C_P2, k).wait_recv()
        x_copy(C_T2, k).start()
        x_copy(C_M2, j).wait_recv()
        x_copy(C_TM2, j).start()

    def last_near(j):
        k = flip(N_CHUNK - 1)
        pair(P1, k, R_P1, T1, k, R_T1, M2, j * TILE, TILE)

    def far_pair(i):
        q = jnp.where(far == 0, flip(i), i)
        pair(far_l, q, R_FAR, far_t, q, R_TFAR, far_w, far * (n_rows // 2), n_rows // 2)

    def far_step(j, _):
        k = flip(j)
        arrive(j)
        mid(j, n_rows // 2)
        last_near(j)
        x_copy(C_T2, k).wait_recv()
        x_copy(C_TM2, j).wait_recv()
        pair(P2, k, R_P2, T2, k, R_T2, M1, 0, n_rows)

        def one(i, _):
            far_pair(i)
            return 0
        lax.fori_loop(jnp.where(j < 3, N_CHUNK, jnp.where(j == 3, 0, j)), jnp.where(j < 3, N_CHUNK, j + 1), one, 0)
        return 0

    lax.fori_loop(0, N_CHUNK - 1, far_step, 0)

    final = N_CHUNK - 1
    arrive(final)
    last_near(final)
    x_copy(C_T2, flip(final)).wait_recv()
    x_copy(C_TM2, final).wait_recv()
    far_pair(final)

    ways = ((T1, partner), (T2, partner), (TM2, partner), (M2, down), (P2, up), (M1, down), (P1, up))
    pieces = range(N_PIECE)

    def back(i, p):
        return r_copy(ways[i][0], i, ways[i][1], p)

    for p in pieces:
        back(2, p).start()
        back(1, p).start()
    for p in pieces:
        back(0, p).start()
    for p in pieces:
        back(2, p).wait_recv()
        acc[M2, :, piece(p)] += rx[2, :, piece(p)]
        back(3, p).start()
        back(1, p).wait_recv()
        acc[P2, :, piece(p)] += rx[1, :, piece(p)]
        back(4, p).start()
    for p in pieces:
        back(0, p).wait_recv()
        acc[P1, :, piece(p)] += rx[0, :, piece(p)]
    for p in pieces:
        back(3, p).wait_recv()
        acc[M1, :, piece(p)] += rx[3, :, piece(p)]
        back(5, p).start()
        back(4, p).wait_recv()
        acc[P1, :, piece(p)] += rx[4, :, piece(p)]
        back(6, p).start()
    for p in pieces:
        back(5, p).wait_recv()
        back(6, p).wait_recv()
        y_ref[:, piece(p)] = acc[OWN, :, piece(p)] + rx[5, :, piece(p)] + rx[6, :, piece(p)]

    def drain(j, _):
        for c in (C_M1, C_P1, C_M2, C_P2, C_T1, C_T2, C_TM2):
            x_copy(c, j).wait_send()
        return 0
    lax.fori_loop(0, N_CHUNK, drain, 0)
    t0_copy().wait_send()
    for c in range(8):
        v_copy(c).wait_send()
        n_copy(c).wait_send()
    for i in range(len(ways)):
        for p in pieces:
            back(i, p).wait_send()


def solution(mesh):
    n_group = mesh.shape['group']
    row_spec = P(('tasks', 'group'), None)

    def local_fn(x_loc, v_loc, lengthscale, outscale):
        n_rows, n_feat = x_loc.shape
        n_rhs = v_loc.shape[1]
        smem = pl.BlockSpec(memory_space=pltpu.SMEM)
        vmem = pl.BlockSpec(memory_space=pltpu.VMEM)

        def body(*refs):
            kernel(n_group, *refs)

        y_t = pl.pallas_call(
            body,
            name='gauss_ring',
            out_shape=jax.ShapeDtypeStruct((n_rhs, n_rows), jnp.float32),
            in_specs=[smem, smem, pl.BlockSpec(memory_space=pl.ANY), vmem],
            out_specs=vmem,
            scratch_shapes=[
                pltpu.VMEM((N_SLOT, n_rows, n_feat), jnp.bfloat16),
                pltpu.VMEM((N_SLOT, n_rhs, n_rows), jnp.bfloat16),
                pltpu.VMEM((N_SLOT, 1, n_rows), jnp.float32),
                pltpu.VMEM((N_REP, n_rows, 128), jnp.float32),
                pltpu.VMEM((N_SLOT, n_rhs, n_rows), jnp.float32),
                pltpu.VMEM((7, n_rhs, n_rows), jnp.float32),
                pltpu.SemaphoreType.DMA((N_CHUNK,)),
                pltpu.SemaphoreType.DMA((7, N_CHUNK)),
                pltpu.SemaphoreType.DMA((7, N_CHUNK)),
                pltpu.SemaphoreType.DMA((8,)),
                pltpu.SemaphoreType.DMA((8,)),
                pltpu.SemaphoreType.DMA((8,)),
                pltpu.SemaphoreType.DMA((8,)),
                pltpu.SemaphoreType.DMA((2,)),
                pltpu.SemaphoreType.DMA((7, N_PIECE)),
                pltpu.SemaphoreType.DMA((7, N_PIECE)),
            ],
            compiler_params=pltpu.CompilerParams(
                collective_id=0, has_side_effects=True, vmem_limit_bytes=58 * 2**20),
        )(lengthscale, outscale, x_loc, v_loc.T)
        return y_t.T

    return jax.shard_map(local_fn, mesh=mesh, in_specs=(row_spec, row_spec, P(None), P(None)), out_specs=row_spec, check_vma=False)
```

```python
import jax
import jax.numpy as jnp
from jax import lax
from jax.experimental import pallas as pl
from jax.experimental.pallas import tpu as pltpu
from jax.sharding import PartitionSpec as P

MESH = pl.DeviceIdType.MESH
LOG2E = 1.4426950408889634
M2, M1, OWN, P1, P2, T0, T1, T2, TM2 = range(9)
N_SLOT = 9
R_OWN, R_T0, R_P1, R_T1, R_P2, R_T2, R_FAR, R_TFAR = range(8)
N_REP = 8
NT = (((1,), (1,)), ((), ()))
NN = (((1,), (0,)), ((), ()))
C_M1, C_P1, C_M2, C_P2, C_T1, C_T2, C_TM2, C_T0 = range(8)
N_CHUNK = 8
TILE = 256
N_PIECE = 4


def dot(a, b, dims):
    return lax.dot_general(a, b, dims, preferred_element_type=jnp.float32)


def kernel(n_group, ell_ref, s_ref, x_ref, v_ref, y_ref, y_vmem, xs, vt, nrm, arep, acc, rx,
           v_sem, y_sem, load_sem, x_send, x_recv, v_send, v_recv, n_send, n_recv, t0_sem, r_send, r_recv):
    n_rows = x_ref.shape[0]
    n_chip = n_group // 2
    me = lax.axis_index('group')
    chip, core = me // 2, me % 2
    up = ((chip + 1) % n_chip) * 2 + core
    down = ((chip + n_chip - 1) % n_chip) * 2 + core
    partner = chip * 2 + 1 - core
    far = chip // (n_chip // 2)
    far_w = M2 + (P2 - M2) * far
    far_l = P2 - (P2 - M2) * far
    far_t = T2 + (TM2 - T2) * far

    def rows_of(j):
        return pl.ds(pl.multiple_of(j * TILE, TILE), TILE)

    def flip(j):
        return (j + N_CHUNK // 2) % N_CHUNK

    SRC = {C_M1: OWN, C_P1: OWN, C_M2: M1, C_P2: P1, C_T1: P1, C_T2: P2, C_TM2: M2, C_T0: OWN}
    DST = {C_M1: M1, C_P1: P1, C_M2: M2, C_P2: P2, C_T1: T1, C_T2: T2, C_TM2: TM2, C_T0: T0}
    TO = {C_M1: up, C_P1: down, C_M2: up, C_P2: down, C_T1: partner, C_T2: partner, C_TM2: partner, C_T0: partner}

    def x_copy(c, j):
        return pltpu.make_async_remote_copy(
            src_ref=xs.at[SRC[c], rows_of(j)], dst_ref=xs.at[DST[c], rows_of(j)],
            send_sem=x_send.at[c, j], recv_sem=x_recv.at[c, j],
            device_id={'group': TO[c]}, device_id_type=MESH)

    def t0_copy():
        return pltpu.make_async_remote_copy(
            src_ref=xs.at[OWN], dst_ref=xs.at[T0], send_sem=t0_sem.at[0], recv_sem=t0_sem.at[1],
            device_id={'group': partner}, device_id_type=MESH)

    def v_copy(c):
        return pltpu.make_async_remote_copy(
            src_ref=vt.at[SRC[c]], dst_ref=vt.at[DST[c]], send_sem=v_send.at[c], recv_sem=v_recv.at[c],
            device_id={'group': TO[c]}, device_id_type=MESH)

    def n_copy(c):
        return pltpu.make_async_remote_copy(
            src_ref=nrm.at[SRC[c]], dst_ref=nrm.at[DST[c]], send_sem=n_send.at[c], recv_sem=n_recv.at[c],
            device_id={'group': TO[c]}, device_id_type=MESH)

    def piece(p):
        return slice(p * n_rows // N_PIECE, (p + 1) * n_rows // N_PIECE)

    def r_copy(src, i, to, p):
        return pltpu.make_async_remote_copy(
            src_ref=acc.at[src, :, piece(p)], dst_ref=rx.at[i, :, piece(p)],
            send_sem=r_send.at[i, p], recv_sem=r_recv.at[i, p],
            device_id={'group': to}, device_id_type=MESH)

    def load(j):
        return pltpu.make_async_copy(x_ref.at[rows_of(j)], xs.at[OWN, rows_of(j)], load_sem.at[j])

    load_v = pltpu.make_async_copy(v_ref, vt.at[OWN], v_sem)
    load_v.start()
    order = [j for i in range(N_CHUNK // 2) for j in (i, flip(i))]
    for j in order:
        load(j).start()
    barrier = pltpu.get_barrier_semaphore()
    for peer in (up, down, partner):
        pl.semaphore_signal(barrier, inc=1, device_id={'group': peer}, device_id_type=MESH)
    pl.semaphore_wait(barrier, 3)
    load_v.wait()
    for c in (C_M1, C_P1, C_T0):
        v_copy(c).start()
    def send_own(first, last):
        for j in range(first, last):
            x_copy(C_M1, j).start()
            x_copy(C_P1, flip(j)).start()

    for j in order[:2]:
        load(j).wait()
    send_own(0, 1)
    for j in order[2:]:
        load(j).wait()
    t0_copy().start()

    ell = jnp.full((1, 128), ell_ref[0], jnp.float32)
    coef = LOG2E / (2.0 * jnp.square(ell))
    top = LOG2E * jnp.log(jnp.full((1, 128), s_ref[0], jnp.float32))

    acc[...] = jnp.zeros_like(acc)

    for b in range(n_rows // 128):
        rows = slice(b * 128, (b + 1) * 128)
        part = jnp.sum(jnp.square(xs[OWN, rows, :].astype(jnp.float32)), axis=1, keepdims=True)
        part = jnp.broadcast_to(part, (128, 128))
        arep[R_OWN, rows, :] = part * coef - top
        nrm[OWN, :, rows] = part.T[0:1, :]
    for c in (C_M1, C_P1, C_T0):
        n_copy(c).start()
    send_own(1, N_CHUNK // 2)

    def column_norms(slot, rep):
        for b in range(n_rows // 128):
            rows = slice(b * 128, (b + 1) * 128)
            row = jnp.broadcast_to(nrm[slot, :, rows], (128, 128))
            arep[rep, rows, :] = row.T * coef - top

    def wide(v, n):
        return jnp.concatenate([v] * (n // 128), axis=1)

    def kern_of(left, shift, w, cols, n):
        gram = dot(left, xs[w, cols, :], NT)
        expo = gram * wide(2.0 * coef, n) - wide(shift, n) - nrm[w, :, cols] * wide(coef, n)
        return jnp.exp2(jnp.minimum(expo, wide(top, n))).astype(jnp.bfloat16)

    def pair(la, ja, ra, lb, jb, rb, w, base, n, sides=True, yw=None):
        cols = pl.ds(pl.multiple_of(base, TILE), n)
        a, b = rows_of(ja), rows_of(jb)
        left = jnp.concatenate([xs[la, a, :], xs[lb, b, :]], axis=0)
        shift = jnp.concatenate([arep[ra, a, :], arep[rb, b, :]], axis=0)
        kern = kern_of(left, shift, w, cols, n)
        v = jnp.concatenate([vt[la, :, a], vt[lb, :, b]], axis=1)
        acc[w, :, cols] += dot(v, kern, NN)
        if sides:
            y = dot(vt[w, :, cols], kern, NT)
            acc[la, :, a] += y[:, :TILE]
            acc[lb, :, b] += y[:, TILE:]

    def own_pairs(slot, rep):
        def one(i, _):
            pair(slot, 2 * i, rep, slot, 2 * i + 1, rep, OWN, 0, n_rows, sides=False)
            return 0
        lax.fori_loop(0, N_CHUNK // 2, one, 0)

    own_pairs(OWN, R_OWN)
    v_copy(C_T0).wait_recv()
    n_copy(C_T0).wait_recv()
    t0_copy().wait_recv()
    column_norms(T0, R_T0)
    own_pairs(T0, R_T0)
    for c in (C_M1, C_P1):
        v_copy(c).wait_recv()
        n_copy(c).wait_recv()
    for c in (C_M2, C_P2, C_T1):
        v_copy(c).start()
        n_copy(c).start()
    send_own(N_CHUNK // 2, N_CHUNK)
    column_norms(P1, R_P1)
    v_copy(C_T1).wait_recv()
    n_copy(C_T1).wait_recv()
    column_norms(T1, R_T1)

    def mid(i, start):
        k = flip(i)
        pair(P1, k, R_P1, T1, k, R_T1, M1, start, n_rows // 2)

    def near_step(j, _):
        @pl.when(j < N_CHUNK)
        def _():
            k = flip(j)
            x_copy(C_P1, k).wait_recv()
            x_copy(C_T1, k).start()
            x_copy(C_P2, k).start()
            x_copy(C_M1, j).wait_recv()
            x_copy(C_M2, j).start()

        @pl.when(j > 0)
        def _():
            i = j - 1
            k = flip(i)
            x_copy(C_T1, k).wait_recv()
            pair(P1, k, R_P1, T1, k, R_T1, OWN, 0, n_rows)

            def one(i, _):
                mid(i, 0)
                return 0
            lax.fori_loop(jnp.where(j < 4, N_CHUNK, jnp.where(j == 4, 0, i)), jnp.where(j < 4, N_CHUNK, j), one, 0)
        return 0

    lax.fori_loop(0, N_CHUNK - 2, near_step, 0)
    for c in (C_M2, C_P2):
        v_copy(c).wait_recv()
        n_copy(c).wait_recv()
    for c in (C_T2, C_TM2):
        v_copy(c).start()
        n_copy(c).start()
    column_norms(P2, R_P2)
    for c in (C_T2, C_TM2):
        v_copy(c).wait_recv()
        n_copy(c).wait_recv()
    column_norms(T2, R_T2)
    column_norms(far_l, R_FAR)
    column_norms(far_t, R_TFAR)
    lax.fori_loop(N_CHUNK - 2, N_CHUNK + 1, near_step, 0)

    mid(N_CHUNK - 1, n_rows // 2)

    def arrive(j):
        k = flip(j)
        x_copy(C_P2, k).wait_recv()
        x_copy(C_T2, k).start()
        x_copy(C_M2, j).wait_recv()
        x_copy(C_TM2, j).start()

    def last_near(j):
        k = flip(N_CHUNK - 1)
        pair(P1, k, R_P1, T1, k, R_T1, M2, j * TILE, TILE)

    def far_pair(i):
        q = jnp.where(far == 0, flip(i), i)
        pair(far_l, q, R_FAR, far_t, q, R_TFAR, far_w, far * (n_rows // 2), n_rows // 2)

    def far_step(j, _):
        k = flip(j)
        arrive(j)
        mid(j, n_rows // 2)
        last_near(j)
        x_copy(C_T2, k).wait_recv()
        x_copy(C_TM2, j).wait_recv()
        pair(P2, k, R_P2, T2, k, R_T2, M1, 0, n_rows)

        def one(i, _):
            far_pair(i)
            return 0
        lax.fori_loop(jnp.where(j < 3, N_CHUNK, jnp.where(j == 3, 0, j)), jnp.where(j < 3, N_CHUNK, j + 1), one, 0)
        return 0

    lax.fori_loop(0, N_CHUNK - 1, far_step, 0)

    final = N_CHUNK - 1
    arrive(final)
    last_near(final)
    x_copy(C_T2, flip(final)).wait_recv()
    x_copy(C_TM2, final).wait_recv()
    far_pair(final)

    ways = ((T1, partner), (T2, partner), (TM2, partner), (M2, down), (P2, up), (M1, down), (P1, up))
    pieces = range(N_PIECE)

    def y_out(p):
        return pltpu.make_async_copy(y_vmem.at[:, piece(p)], y_ref.at[:, piece(p)], y_sem.at[p])

    def back(i, p):
        return r_copy(ways[i][0], i, ways[i][1], p)

    for p in pieces:
        back(2, p).start()
        back(1, p).start()
    for p in pieces:
        back(0, p).start()
    for p in pieces:
        back(2, p).wait_recv()
        acc[M2, :, piece(p)] += rx[2, :, piece(p)]
        back(3, p).start()
        back(1, p).wait_recv()
        acc[P2, :, piece(p)] += rx[1, :, piece(p)]
        back(4, p).start()
    for p in pieces:
        back(0, p).wait_recv()
        acc[P1, :, piece(p)] += rx[0, :, piece(p)]
    for p in pieces:
        back(3, p).wait_recv()
        acc[M1, :, piece(p)] += rx[3, :, piece(p)]
        back(5, p).start()
        back(4, p).wait_recv()
        acc[P1, :, piece(p)] += rx[4, :, piece(p)]
        back(6, p).start()
    for p in pieces:
        back(5, p).wait_recv()
        back(6, p).wait_recv()
        y_vmem[:, piece(p)] = acc[OWN, :, piece(p)] + rx[5, :, piece(p)] + rx[6, :, piece(p)]
        y_out(p).start()

    def drain(j, _):
        for c in (C_M1, C_P1, C_M2, C_P2, C_T1, C_T2, C_TM2):
            x_copy(c, j).wait_send()
        return 0
    lax.fori_loop(0, N_CHUNK, drain, 0)
    t0_copy().wait_send()
    for c in range(8):
        v_copy(c).wait_send()
        n_copy(c).wait_send()
    for i in range(len(ways)):
        for p in pieces:
            back(i, p).wait_send()
    for p in pieces:
        y_out(p).wait()


def solution(mesh):
    n_group = mesh.shape['group']
    row_spec = P(('tasks', 'group'), None)

    def local_fn(x_loc, v_loc, lengthscale, outscale):
        n_rows, n_feat = x_loc.shape
        n_rhs = v_loc.shape[1]
        smem = pl.BlockSpec(memory_space=pltpu.SMEM)
        hbm = pl.BlockSpec(memory_space=pl.ANY)

        def body(*refs):
            kernel(n_group, *refs)

        y_t = pl.pallas_call(
            body,
            name='gauss_ring',
            out_shape=jax.ShapeDtypeStruct((n_rhs, n_rows), jnp.float32),
            in_specs=[smem, smem, hbm, hbm],
            out_specs=hbm,
            scratch_shapes=[
                pltpu.VMEM((n_rhs, n_rows), jnp.float32),
                pltpu.VMEM((N_SLOT, n_rows, n_feat), jnp.bfloat16),
                pltpu.VMEM((N_SLOT, n_rhs, n_rows), jnp.bfloat16),
                pltpu.VMEM((N_SLOT, 1, n_rows), jnp.float32),
                pltpu.VMEM((N_REP, n_rows, 128), jnp.float32),
                pltpu.VMEM((N_SLOT, n_rhs, n_rows), jnp.float32),
                pltpu.VMEM((7, n_rhs, n_rows), jnp.float32),
                pltpu.SemaphoreType.DMA,
                pltpu.SemaphoreType.DMA((N_PIECE,)),
                pltpu.SemaphoreType.DMA((N_CHUNK,)),
                pltpu.SemaphoreType.DMA((7, N_CHUNK)),
                pltpu.SemaphoreType.DMA((7, N_CHUNK)),
                pltpu.SemaphoreType.DMA((8,)),
                pltpu.SemaphoreType.DMA((8,)),
                pltpu.SemaphoreType.DMA((8,)),
                pltpu.SemaphoreType.DMA((8,)),
                pltpu.SemaphoreType.DMA((2,)),
                pltpu.SemaphoreType.DMA((7, N_PIECE)),
                pltpu.SemaphoreType.DMA((7, N_PIECE)),
            ],
            compiler_params=pltpu.CompilerParams(
                collective_id=0, has_side_effects=True, vmem_limit_bytes=58 * 2**20),
        )(lengthscale, outscale, x_loc, v_loc.T)
        return y_t.T

    return jax.shard_map(local_fn, mesh=mesh, in_specs=(row_spec, row_spec, P(None), P(None)), out_specs=row_spec, check_vma=False)
```

```python
import jax
import jax.numpy as jnp
from jax import lax
from jax.experimental import pallas as pl
from jax.experimental.pallas import tpu as pltpu
from jax.sharding import PartitionSpec as P

MESH = pl.DeviceIdType.MESH
LOG2E = 1.4426950408889634
M2, M1, OWN, P1, P2, T0, T1, T2, TM2 = range(9)
N_SLOT = 9
R_OWN, R_T0, R_P1, R_T1, R_P2, R_T2, R_FAR, R_TFAR = range(8)
N_REP = 8
NT = (((1,), (1,)), ((), ()))
NN = (((1,), (0,)), ((), ()))
C_M1, C_P1, C_M2, C_P2, C_T1, C_T2, C_TM2, C_T0 = range(8)
N_CHUNK = 8
TILE = 256
N_PIECE = 4


def dot(a, b, dims):
    return lax.dot_general(a, b, dims, preferred_element_type=jnp.float32)


def kernel(n_group, ell_ref, s_ref, x_ref, v_ref, y_ref, y_vmem, xs, vt, nrm, arep, acc, rx,
           v_sem, y_sem, load_sem, x_send, x_recv, v_send, v_recv, n_send, n_recv, t0_sem, r_send, r_recv):
    n_rows = x_ref.shape[0]
    n_chip = n_group // 2
    me = lax.axis_index('group')
    chip, core = me // 2, me % 2
    up = ((chip + 1) % n_chip) * 2 + core
    down = ((chip + n_chip - 1) % n_chip) * 2 + core
    partner = chip * 2 + 1 - core
    far = chip // (n_chip // 2)
    far_w = M2 + (P2 - M2) * far
    far_l = P2 - (P2 - M2) * far
    far_t = T2 + (TM2 - T2) * far

    def rows_of(j):
        return pl.ds(pl.multiple_of(j * TILE, TILE), TILE)

    def flip(j):
        return (j + N_CHUNK // 2) % N_CHUNK

    SRC = {C_M1: OWN, C_P1: OWN, C_M2: M1, C_P2: P1, C_T1: P1, C_T2: P2, C_TM2: M2, C_T0: OWN}
    DST = {C_M1: M1, C_P1: P1, C_M2: M2, C_P2: P2, C_T1: T1, C_T2: T2, C_TM2: TM2, C_T0: T0}
    TO = {C_M1: up, C_P1: down, C_M2: up, C_P2: down, C_T1: partner, C_T2: partner, C_TM2: partner, C_T0: partner}

    def x_copy(c, j):
        return pltpu.make_async_remote_copy(
            src_ref=xs.at[SRC[c], rows_of(j)], dst_ref=xs.at[DST[c], rows_of(j)],
            send_sem=x_send.at[c, j], recv_sem=x_recv.at[c, j],
            device_id={'group': TO[c]}, device_id_type=MESH)

    def t0_copy():
        return pltpu.make_async_remote_copy(
            src_ref=xs.at[OWN], dst_ref=xs.at[T0], send_sem=t0_sem.at[0], recv_sem=t0_sem.at[1],
            device_id={'group': partner}, device_id_type=MESH)

    def v_copy(c):
        return pltpu.make_async_remote_copy(
            src_ref=vt.at[SRC[c]], dst_ref=vt.at[DST[c]], send_sem=v_send.at[c], recv_sem=v_recv.at[c],
            device_id={'group': TO[c]}, device_id_type=MESH)

    def n_copy(c):
        return pltpu.make_async_remote_copy(
            src_ref=nrm.at[SRC[c]], dst_ref=nrm.at[DST[c]], send_sem=n_send.at[c], recv_sem=n_recv.at[c],
            device_id={'group': TO[c]}, device_id_type=MESH)

    def piece(p):
        return slice(p * n_rows // N_PIECE, (p + 1) * n_rows // N_PIECE)

    def r_copy(src, i, to, p):
        return pltpu.make_async_remote_copy(
            src_ref=acc.at[src, :, piece(p)], dst_ref=rx.at[i, :, piece(p)],
            send_sem=r_send.at[i, p], recv_sem=r_recv.at[i, p],
            device_id={'group': to}, device_id_type=MESH)

    def load(j):
        return pltpu.make_async_copy(x_ref.at[rows_of(j)], xs.at[OWN, rows_of(j)], load_sem.at[j])

    load_v = pltpu.make_async_copy(v_ref, vt.at[OWN], v_sem)
    load_v.start()
    order = [j for i in range(N_CHUNK // 2) for j in (i, flip(i))]
    for j in order:
        load(j).start()
    barrier = pltpu.get_barrier_semaphore()
    for peer in (up, down, partner):
        pl.semaphore_signal(barrier, inc=1, device_id={'group': peer}, device_id_type=MESH)
    pl.semaphore_wait(barrier, 3)
    load_v.wait()
    for c in (C_M1, C_P1, C_T0):
        v_copy(c).start()
    def send_own(first, last):
        for j in range(first, last):
            x_copy(C_M1, j).start()
            x_copy(C_P1, flip(j)).start()

    for j in order[:2]:
        load(j).wait()
    send_own(0, 1)
    for j in order[2:]:
        load(j).wait()
    t0_copy().start()

    ell = jnp.full((1, 128), ell_ref[0], jnp.float32)
    coef = LOG2E / (2.0 * jnp.square(ell))
    top = LOG2E * jnp.log(jnp.full((1, 128), s_ref[0], jnp.float32))

    acc[...] = jnp.zeros_like(acc)

    for b in range(n_rows // 128):
        rows = slice(b * 128, (b + 1) * 128)
        part = jnp.sum(jnp.square(xs[OWN, rows, :].astype(jnp.float32)), axis=1, keepdims=True)
        part = jnp.broadcast_to(part, (128, 128))
        arep[R_OWN, rows, :] = part * coef - top
        nrm[OWN, :, rows] = part.T[0:1, :]
    for c in (C_M1, C_P1, C_T0):
        n_copy(c).start()
    send_own(1, N_CHUNK // 2)

    def column_norms(slot, rep):
        for b in range(n_rows // 128):
            rows = slice(b * 128, (b + 1) * 128)
            row = jnp.broadcast_to(nrm[slot, :, rows], (128, 128))
            arep[rep, rows, :] = row.T * coef - top

    def wide(v, n):
        return jnp.concatenate([v] * (n // 128), axis=1)

    def kern_of(left, shift, w, cols, n):
        gram = dot(left, xs[w, cols, :], NT)
        expo = gram * wide(2.0 * coef, n) - wide(shift, n) - nrm[w, :, cols] * wide(coef, n)
        return jnp.exp2(jnp.minimum(expo, wide(top, n))).astype(jnp.bfloat16)

    def pair(la, ja, ra, lb, jb, rb, w, base, n, sides=True, yw=None):
        cols = pl.ds(pl.multiple_of(base, TILE), n)
        a, b = rows_of(ja), rows_of(jb)
        left = jnp.concatenate([xs[la, a, :], xs[lb, b, :]], axis=0)
        shift = jnp.concatenate([arep[ra, a, :], arep[rb, b, :]], axis=0)
        kern = kern_of(left, shift, w, cols, n)
        v = jnp.concatenate([vt[la, :, a], vt[lb, :, b]], axis=1)
        acc[w, :, cols] += dot(v, kern, NN)
        if sides:
            y = dot(vt[w, :, cols], kern, NT)
            acc[la, :, a] += y[:, :TILE]
            acc[lb, :, b] += y[:, TILE:]

    def own_pairs(slot, rep):
        def one(i, _):
            pair(slot, 2 * i, rep, slot, 2 * i + 1, rep, OWN, 0, n_rows, sides=False)
            return 0
        lax.fori_loop(0, N_CHUNK // 2, one, 0)

    own_pairs(OWN, R_OWN)
    v_copy(C_T0).wait_recv()
    n_copy(C_T0).wait_recv()
    t0_copy().wait_recv()
    column_norms(T0, R_T0)
    own_pairs(T0, R_T0)
    for c in (C_M1, C_P1):
        v_copy(c).wait_recv()
        n_copy(c).wait_recv()
    for c in (C_M2, C_P2, C_T1):
        v_copy(c).start()
        n_copy(c).start()
    send_own(N_CHUNK // 2, N_CHUNK)
    column_norms(P1, R_P1)
    v_copy(C_T1).wait_recv()
    n_copy(C_T1).wait_recv()
    column_norms(T1, R_T1)

    def mid(i, start):
        k = flip(i)
        pair(P1, k, R_P1, T1, k, R_T1, M1, start, n_rows // 2)

    def near_step(j, _):
        @pl.when(j < N_CHUNK)
        def _():
            k = flip(j)
            x_copy(C_P1, k).wait_recv()
            x_copy(C_T1, k).start()
            x_copy(C_P2, k).start()
            x_copy(C_M1, j).wait_recv()
            x_copy(C_M2, j).start()

        @pl.when(j > 0)
        def _():
            i = j - 1
            k = flip(i)
            x_copy(C_T1, k).wait_recv()
            pair(P1, k, R_P1, T1, k, R_T1, OWN, 0, n_rows)

            def one(i, _):
                mid(i, 0)
                return 0
            lax.fori_loop(jnp.where(j < 4, N_CHUNK, jnp.where(j == 4, 0, i)), jnp.where(j < 4, N_CHUNK, j), one, 0)
        return 0

    lax.fori_loop(0, N_CHUNK - 2, near_step, 0)
    for c in (C_M2, C_P2):
        v_copy(c).wait_recv()
        n_copy(c).wait_recv()
    for c in (C_T2, C_TM2):
        v_copy(c).start()
        n_copy(c).start()
    column_norms(P2, R_P2)
    for c in (C_T2, C_TM2):
        v_copy(c).wait_recv()
        n_copy(c).wait_recv()
    column_norms(T2, R_T2)
    column_norms(far_l, R_FAR)
    column_norms(far_t, R_TFAR)
    lax.fori_loop(N_CHUNK - 2, N_CHUNK + 1, near_step, 0)

    mid(N_CHUNK - 1, n_rows // 2)

    def arrive(j):
        k = flip(j)
        x_copy(C_P2, k).wait_recv()
        x_copy(C_T2, k).start()
        x_copy(C_M2, j).wait_recv()
        x_copy(C_TM2, j).start()

    def last_near(j):
        k = flip(N_CHUNK - 1)
        pair(P1, k, R_P1, T1, k, R_T1, M2, j * TILE, TILE)

    def far_pair(i):
        q = jnp.where(far == 0, flip(i), i)
        pair(far_l, q, R_FAR, far_t, q, R_TFAR, far_w, far * (n_rows // 2), n_rows // 2)

    def far_step(j, _):
        k = flip(j)
        arrive(j)
        mid(j, n_rows // 2)
        last_near(j)
        x_copy(C_T2, k).wait_recv()
        x_copy(C_TM2, j).wait_recv()
        pair(P2, k, R_P2, T2, k, R_T2, M1, 0, n_rows)

        def one(i, _):
            far_pair(i)
            return 0
        lax.fori_loop(jnp.where(j < 3, N_CHUNK, jnp.where(j == 3, 0, j)), jnp.where(j < 3, N_CHUNK, j + 1), one, 0)
        return 0

    lax.fori_loop(0, N_CHUNK - 1, far_step, 0)

    ways = ((T1, partner), (T2, partner), (TM2, partner), (M2, down), (P2, up), (M1, down), (P1, up))
    B_T1, B_T2, B_TM2, B_M2, B_P2, B_M1, B_P1 = range(7)
    pieces = range(N_PIECE)

    def y_out(p):
        return pltpu.make_async_copy(y_vmem.at[:, piece(p)], y_ref.at[:, piece(p)], y_sem.at[p])

    def back(i, p):
        return r_copy(ways[i][0], i, ways[i][1], p)

    def take(i, p, slot):
        back(i, p).wait_recv()
        acc[slot, :, piece(p)] += rx[i, :, piece(p)]

    early = {B_TM2: (2, 0, 1), B_T2: (0, 2, 3), B_T1: (0, 2, 3)}
    late = {B_TM2: 3, B_T2: 1, B_T1: 1}
    home = {B_TM2: M2, B_T2: P2, B_T1: P1}
    for i in early:
        for p in early[i]:
            back(i, p).start()
    final = N_CHUNK - 1
    arrive(final)
    for i in early:
        for p in early[i]:
            take(i, p, home[i])
    back(B_M2, 2).start()
    back(B_P2, 0).start()
    last_near(final)
    x_copy(C_T2, flip(final)).wait_recv()
    x_copy(C_TM2, final).wait_recv()
    far_pair(final)
    for i in late:
        back(i, late[i]).start()
    for p, q in ((0, 2), (1, 3)):
        back(B_M2, p).start()
        back(B_P2, q).start()
    take(B_TM2, 3, M2)
    back(B_M2, 3).start()
    take(B_T2, 1, P2)
    back(B_P2, 1).start()
    take(B_T1, 1, P1)
    for p, q in ((2, 0), (0, 2), (1, 3), (3, 1)):
        take(B_M2, p, M1)
        back(B_M1, p).start()
        take(B_P2, q, P1)
        back(B_P1, q).start()
    for p in (0, 2, 1, 3):
        back(B_M1, p).wait_recv()
        back(B_P1, p).wait_recv()
        y_vmem[:, piece(p)] = acc[OWN, :, piece(p)] + rx[B_M1, :, piece(p)] + rx[B_P1, :, piece(p)]
        y_out(p).start()

    def drain(j, _):
        for c in (C_M1, C_P1, C_M2, C_P2, C_T1, C_T2, C_TM2):
            x_copy(c, j).wait_send()
        return 0
    lax.fori_loop(0, N_CHUNK, drain, 0)
    t0_copy().wait_send()
    for c in range(8):
        v_copy(c).wait_send()
        n_copy(c).wait_send()
    for i in range(len(ways)):
        for p in pieces:
            back(i, p).wait_send()
    for p in pieces:
        y_out(p).wait()


def solution(mesh):
    n_group = mesh.shape['group']
    row_spec = P(('tasks', 'group'), None)

    def local_fn(x_loc, v_loc, lengthscale, outscale):
        n_rows, n_feat = x_loc.shape
        n_rhs = v_loc.shape[1]
        smem = pl.BlockSpec(memory_space=pltpu.SMEM)
        hbm = pl.BlockSpec(memory_space=pl.ANY)

        def body(*refs):
            kernel(n_group, *refs)

        y_t = pl.pallas_call(
            body,
            name='gauss_ring',
            out_shape=jax.ShapeDtypeStruct((n_rhs, n_rows), jnp.float32),
            in_specs=[smem, smem, hbm, hbm],
            out_specs=hbm,
            scratch_shapes=[
                pltpu.VMEM((n_rhs, n_rows), jnp.float32),
                pltpu.VMEM((N_SLOT, n_rows, n_feat), jnp.bfloat16),
                pltpu.VMEM((N_SLOT, n_rhs, n_rows), jnp.bfloat16),
                pltpu.VMEM((N_SLOT, 1, n_rows), jnp.float32),
                pltpu.VMEM((N_REP, n_rows, 128), jnp.float32),
                pltpu.VMEM((N_SLOT, n_rhs, n_rows), jnp.float32),
                pltpu.VMEM((7, n_rhs, n_rows), jnp.float32),
                pltpu.SemaphoreType.DMA,
                pltpu.SemaphoreType.DMA((N_PIECE,)),
                pltpu.SemaphoreType.DMA((N_CHUNK,)),
                pltpu.SemaphoreType.DMA((7, N_CHUNK)),
                pltpu.SemaphoreType.DMA((7, N_CHUNK)),
                pltpu.SemaphoreType.DMA((8,)),
                pltpu.SemaphoreType.DMA((8,)),
                pltpu.SemaphoreType.DMA((8,)),
                pltpu.SemaphoreType.DMA((8,)),
                pltpu.SemaphoreType.DMA((2,)),
                pltpu.SemaphoreType.DMA((7, N_PIECE)),
                pltpu.SemaphoreType.DMA((7, N_PIECE)),
            ],
            compiler_params=pltpu.CompilerParams(
                collective_id=0, has_side_effects=True, vmem_limit_bytes=58 * 2**20),
        )(lengthscale, outscale, x_loc, v_loc.T)
        return y_t.T

    return jax.shard_map(local_fn, mesh=mesh, in_specs=(row_spec, row_spec, P(None), P(None)), out_specs=row_spec, check_vma=False)
```

```python
import jax
import jax.numpy as jnp
from jax import lax
from jax.experimental import pallas as pl
from jax.experimental.pallas import tpu as pltpu
from jax.sharding import PartitionSpec as P

MESH = pl.DeviceIdType.MESH
LOG2E = 1.4426950408889634
M2, M1, OWN, P1, P2, T0, T1, T2, TM2 = range(9)
N_SLOT = 9
R_OWN, R_T0, R_P1, R_T1, R_P2, R_T2, R_FAR, R_TFAR = range(8)
N_REP = 8
NT = (((1,), (1,)), ((), ()))
NN = (((1,), (0,)), ((), ()))
C_M1, C_P1, C_M2, C_P2, C_T1, C_T2, C_TM2, C_T0 = range(8)
N_CHUNK = 8
TILE = 256
N_PIECE = 4


def dot(a, b, dims):
    return lax.dot_general(a, b, dims, preferred_element_type=jnp.float32)


def kernel(n_group, ell_ref, s_ref, x_ref, v_ref, y_ref, y_vmem, xs, vt, nrm, arep, acc, rx,
           v_sem, y_sem, load_sem, x_send, x_recv, v_send, v_recv, n_send, n_recv, t0_sem, r_send, r_recv):
    n_rows = x_ref.shape[0]
    n_chip = n_group // 2
    me = lax.axis_index('group')
    chip, core = me // 2, me % 2
    up = ((chip + 1) % n_chip) * 2 + core
    down = ((chip + n_chip - 1) % n_chip) * 2 + core
    partner = chip * 2 + 1 - core
    far = chip // (n_chip // 2)
    far_w = M2 + (P2 - M2) * far
    far_l = P2 - (P2 - M2) * far
    far_t = T2 + (TM2 - T2) * far

    def rows_of(j):
        return pl.ds(pl.multiple_of(j * TILE, TILE), TILE)

    def flip(j):
        return (j + N_CHUNK // 2) % N_CHUNK

    SRC = {C_M1: OWN, C_P1: OWN, C_M2: M1, C_P2: P1, C_T1: P1, C_T2: P2, C_TM2: M2, C_T0: OWN}
    DST = {C_M1: M1, C_P1: P1, C_M2: M2, C_P2: P2, C_T1: T1, C_T2: T2, C_TM2: TM2, C_T0: T0}
    TO = {C_M1: up, C_P1: down, C_M2: up, C_P2: down, C_T1: partner, C_T2: partner, C_TM2: partner, C_T0: partner}

    def x_copy(c, j):
        return pltpu.make_async_remote_copy(
            src_ref=xs.at[SRC[c], rows_of(j)], dst_ref=xs.at[DST[c], rows_of(j)],
            send_sem=x_send.at[c, j], recv_sem=x_recv.at[c, j],
            device_id={'group': TO[c]}, device_id_type=MESH)

    def t0_copy():
        return pltpu.make_async_remote_copy(
            src_ref=xs.at[OWN], dst_ref=xs.at[T0], send_sem=t0_sem.at[0], recv_sem=t0_sem.at[1],
            device_id={'group': partner}, device_id_type=MESH)

    def v_copy(c):
        return pltpu.make_async_remote_copy(
            src_ref=vt.at[SRC[c]], dst_ref=vt.at[DST[c]], send_sem=v_send.at[c], recv_sem=v_recv.at[c],
            device_id={'group': TO[c]}, device_id_type=MESH)

    def n_copy(c):
        return pltpu.make_async_remote_copy(
            src_ref=nrm.at[SRC[c]], dst_ref=nrm.at[DST[c]], send_sem=n_send.at[c], recv_sem=n_recv.at[c],
            device_id={'group': TO[c]}, device_id_type=MESH)

    def piece(p):
        return slice(p * n_rows // N_PIECE, (p + 1) * n_rows // N_PIECE)

    def r_copy(src, i, to, p):
        return pltpu.make_async_remote_copy(
            src_ref=acc.at[src, :, piece(p)], dst_ref=rx.at[i, :, piece(p)],
            send_sem=r_send.at[i, p], recv_sem=r_recv.at[i, p],
            device_id={'group': to}, device_id_type=MESH)

    def load(j):
        return pltpu.make_async_copy(x_ref.at[rows_of(j)], xs.at[OWN, rows_of(j)], load_sem.at[j])

    load_v = pltpu.make_async_copy(v_ref, vt.at[OWN], v_sem)
    load_v.start()
    order = [j for i in range(N_CHUNK // 2) for j in (i, flip(i))]
    for j in order:
        load(j).start()
    barrier = pltpu.get_barrier_semaphore()
    for peer in (up, down, partner):
        pl.semaphore_signal(barrier, inc=1, device_id={'group': peer}, device_id_type=MESH)
    pl.semaphore_wait(barrier, 3)
    load_v.wait()
    for c in (C_M1, C_P1, C_T0):
        v_copy(c).start()
    def send_own(first, last):
        for j in range(first, last):
            x_copy(C_M1, j).start()
            x_copy(C_P1, flip(j)).start()

    for j in order[:2]:
        load(j).wait()
    send_own(0, 1)
    for j in order[2:]:
        load(j).wait()
    t0_copy().start()

    ell = jnp.full((1, 128), ell_ref[0], jnp.float32)
    coef = LOG2E / (2.0 * jnp.square(ell))
    top = LOG2E * jnp.log(jnp.full((1, 128), s_ref[0], jnp.float32))

    acc[...] = jnp.zeros_like(acc)

    for b in range(n_rows // 128):
        rows = slice(b * 128, (b + 1) * 128)
        part = jnp.sum(jnp.square(xs[OWN, rows, :].astype(jnp.float32)), axis=1, keepdims=True)
        part = jnp.broadcast_to(part, (128, 128))
        arep[R_OWN, rows, :] = part * coef - top
        nrm[OWN, :, rows] = part.T[0:1, :]
    for c in (C_M1, C_P1, C_T0):
        n_copy(c).start()
    send_own(1, N_CHUNK // 2)

    def column_norms(slot, rep):
        for b in range(n_rows // 128):
            rows = slice(b * 128, (b + 1) * 128)
            row = jnp.broadcast_to(nrm[slot, :, rows], (128, 128))
            arep[rep, rows, :] = row.T * coef - top

    def wide(v, n):
        return jnp.concatenate([v] * (n // 128), axis=1)

    def kern_of(left, shift, w, cols, n):
        gram = dot(left, xs[w, cols, :], NT)
        expo = gram * wide(2.0 * coef, n) - wide(shift, n) - nrm[w, :, cols] * wide(coef, n)
        return jnp.exp2(jnp.minimum(expo, wide(top, n))).astype(jnp.bfloat16)

    def pair(la, ja, ra, lb, jb, rb, w, base, n, sides=True, yw=None):
        cols = pl.ds(pl.multiple_of(base, TILE), n)
        a, b = rows_of(ja), rows_of(jb)
        left = jnp.concatenate([xs[la, a, :], xs[lb, b, :]], axis=0)
        shift = jnp.concatenate([arep[ra, a, :], arep[rb, b, :]], axis=0)
        kern = kern_of(left, shift, w, cols, n)
        v = jnp.concatenate([vt[la, :, a], vt[lb, :, b]], axis=1)
        acc[w, :, cols] += dot(v, kern, NN)
        if sides:
            y = dot(vt[w, :, cols], kern, NT)
            acc[la, :, a] += y[:, :TILE]
            acc[lb, :, b] += y[:, TILE:]

    def own_pairs(slot, rep):
        def one(i, _):
            pair(slot, 2 * i, rep, slot, 2 * i + 1, rep, OWN, 0, n_rows, sides=False)
            return 0
        lax.fori_loop(0, N_CHUNK // 2, one, 0)

    own_pairs(OWN, R_OWN)
    v_copy(C_T0).wait_recv()
    n_copy(C_T0).wait_recv()
    t0_copy().wait_recv()
    column_norms(T0, R_T0)
    own_pairs(T0, R_T0)
    for c in (C_M1, C_P1):
        v_copy(c).wait_recv()
        n_copy(c).wait_recv()
    for c in (C_M2, C_P2, C_T1):
        v_copy(c).start()
        n_copy(c).start()
    send_own(N_CHUNK // 2, N_CHUNK)
    column_norms(P1, R_P1)
    v_copy(C_T1).wait_recv()
    n_copy(C_T1).wait_recv()
    column_norms(T1, R_T1)

    def mid(i, start):
        k = flip(i)
        pair(P1, k, R_P1, T1, k, R_T1, M1, start, n_rows // 2)

    def near_step(j, _):
        @pl.when(j < N_CHUNK)
        def _():
            k = flip(j)
            x_copy(C_P1, k).wait_recv()
            x_copy(C_T1, k).start()
            x_copy(C_P2, k).start()
            x_copy(C_M1, j).wait_recv()
            x_copy(C_M2, j).start()

        @pl.when(j > 0)
        def _():
            i = j - 1
            k = flip(i)
            x_copy(C_T1, k).wait_recv()
            pair(P1, k, R_P1, T1, k, R_T1, OWN, 0, n_rows)

            def one(i, _):
                mid(i, 0)
                return 0
            lax.fori_loop(jnp.where(j < 4, N_CHUNK, jnp.where(j == 4, 0, i)), jnp.where(j < 4, N_CHUNK, j), one, 0)
        return 0

    lax.fori_loop(0, N_CHUNK - 2, near_step, 0)
    for c in (C_M2, C_P2):
        v_copy(c).wait_recv()
        n_copy(c).wait_recv()
    for c in (C_T2, C_TM2):
        v_copy(c).start()
        n_copy(c).start()
    column_norms(P2, R_P2)
    for c in (C_T2, C_TM2):
        v_copy(c).wait_recv()
        n_copy(c).wait_recv()
    column_norms(T2, R_T2)
    column_norms(far_l, R_FAR)
    column_norms(far_t, R_TFAR)
    lax.fori_loop(N_CHUNK - 2, N_CHUNK + 1, near_step, 0)

    mid(N_CHUNK - 1, n_rows // 2)

    def arrive(j):
        k = flip(j)
        x_copy(C_P2, k).wait_recv()
        x_copy(C_T2, k).start()
        x_copy(C_M2, j).wait_recv()
        x_copy(C_TM2, j).start()

    def last_near(j):
        k = flip(N_CHUNK - 1)
        pair(P1, k, R_P1, T1, k, R_T1, M2, j * TILE, TILE)

    def far_pair(i):
        q = jnp.where(far == 0, flip(i), i)
        pair(far_l, q, R_FAR, far_t, q, R_TFAR, far_w, far * (n_rows // 2), n_rows // 2)

    def far_single(slot, j, rep):
        n = n_rows // 2
        cols = pl.ds(pl.multiple_of(far * n, TILE), n)
        a = rows_of(j)
        kern = kern_of(xs[slot, a, :], arep[rep, a, :], far_w, cols, n)
        acc[far_w, :, cols] += dot(vt[slot, :, a], kern, NN)
        acc[slot, :, a] += dot(vt[far_w, :, cols], kern, NT)

    def far_step(j, _):
        k = flip(j)
        arrive(j)
        mid(j, n_rows // 2)
        last_near(j)
        x_copy(C_T2, k).wait_recv()
        x_copy(C_TM2, j).wait_recv()
        pair(P2, k, R_P2, T2, k, R_T2, M1, 0, n_rows)

        def one(i, _):
            far_pair(i)
            return 0
        lax.fori_loop(jnp.where(j < 3, N_CHUNK, jnp.where(j == 3, 0, j)), jnp.where(j < 3, N_CHUNK, j + 1), one, 0)
        return 0

    lax.fori_loop(0, N_CHUNK - 1, far_step, 0)

    ways = ((T1, partner), (T2, partner), (TM2, partner), (M2, down), (P2, up), (M1, down), (P1, up))
    B_T1, B_T2, B_TM2, B_M2, B_P2, B_M1, B_P1 = range(7)
    pieces = range(N_PIECE)

    def y_out(p):
        return pltpu.make_async_copy(y_vmem.at[:, piece(p)], y_ref.at[:, piece(p)], y_sem.at[p])

    def back(i, p):
        return r_copy(ways[i][0], i, ways[i][1], p)

    def take(i, p, slot):
        back(i, p).wait_recv()
        acc[slot, :, piece(p)] += rx[i, :, piece(p)]

    early = {B_TM2: (2, 0, 1), B_T2: (0, 2, 3), B_T1: (0, 2, 3)}
    late = {B_TM2: 3, B_T2: 1, B_T1: 1}
    home = {B_TM2: M2, B_T2: P2, B_T1: P1}
    for i in early:
        for p in early[i]:
            back(i, p).start()
    final = N_CHUNK - 1
    arrive(final)
    for i in early:
        for p in early[i]:
            take(i, p, home[i])
    back(B_M2, 2).start()
    back(B_P2, 0).start()
    last_near(final)
    last = jnp.where(far == 0, flip(final), final)
    far_single(far_l, last, R_FAR)
    x_copy(C_T2, flip(final)).wait_recv()
    x_copy(C_TM2, final).wait_recv()
    far_single(far_t, last, R_TFAR)
    for i in late:
        back(i, late[i]).start()
    for p, q in ((0, 2), (1, 3)):
        back(B_M2, p).start()
        back(B_P2, q).start()
    take(B_TM2, 3, M2)
    back(B_M2, 3).start()
    take(B_T2, 1, P2)
    back(B_P2, 1).start()
    take(B_T1, 1, P1)
    for p, q in ((2, 0), (0, 2), (1, 3), (3, 1)):
        take(B_M2, p, M1)
        back(B_M1, p).start()
        take(B_P2, q, P1)
        back(B_P1, q).start()
    for p in (0, 2, 1, 3):
        back(B_M1, p).wait_recv()
        back(B_P1, p).wait_recv()
        y_vmem[:, piece(p)] = acc[OWN, :, piece(p)] + rx[B_M1, :, piece(p)] + rx[B_P1, :, piece(p)]
        y_out(p).start()

    def drain(j, _):
        for c in (C_M1, C_P1, C_M2, C_P2, C_T1, C_T2, C_TM2):
            x_copy(c, j).wait_send()
        return 0
    lax.fori_loop(0, N_CHUNK, drain, 0)
    t0_copy().wait_send()
    for c in range(8):
        v_copy(c).wait_send()
        n_copy(c).wait_send()
    for i in range(len(ways)):
        for p in pieces:
            back(i, p).wait_send()
    for p in pieces:
        y_out(p).wait()


def solution(mesh):
    n_group = mesh.shape['group']
    row_spec = P(('tasks', 'group'), None)

    def local_fn(x_loc, v_loc, lengthscale, outscale):
        n_rows, n_feat = x_loc.shape
        n_rhs = v_loc.shape[1]
        smem = pl.BlockSpec(memory_space=pltpu.SMEM)
        hbm = pl.BlockSpec(memory_space=pl.ANY)

        def body(*refs):
            kernel(n_group, *refs)

        y_t = pl.pallas_call(
            body,
            name='gauss_ring',
            out_shape=jax.ShapeDtypeStruct((n_rhs, n_rows), jnp.float32),
            in_specs=[smem, smem, hbm, hbm],
            out_specs=hbm,
            scratch_shapes=[
                pltpu.VMEM((n_rhs, n_rows), jnp.float32),
                pltpu.VMEM((N_SLOT, n_rows, n_feat), jnp.bfloat16),
                pltpu.VMEM((N_SLOT, n_rhs, n_rows), jnp.bfloat16),
                pltpu.VMEM((N_SLOT, 1, n_rows), jnp.float32),
                pltpu.VMEM((N_REP, n_rows, 128), jnp.float32),
                pltpu.VMEM((N_SLOT, n_rhs, n_rows), jnp.float32),
                pltpu.VMEM((7, n_rhs, n_rows), jnp.float32),
                pltpu.SemaphoreType.DMA,
                pltpu.SemaphoreType.DMA((N_PIECE,)),
                pltpu.SemaphoreType.DMA((N_CHUNK,)),
                pltpu.SemaphoreType.DMA((7, N_CHUNK)),
                pltpu.SemaphoreType.DMA((7, N_CHUNK)),
                pltpu.SemaphoreType.DMA((8,)),
                pltpu.SemaphoreType.DMA((8,)),
                pltpu.SemaphoreType.DMA((8,)),
                pltpu.SemaphoreType.DMA((8,)),
                pltpu.SemaphoreType.DMA((2,)),
                pltpu.SemaphoreType.DMA((7, N_PIECE)),
                pltpu.SemaphoreType.DMA((7, N_PIECE)),
            ],
            compiler_params=pltpu.CompilerParams(
                collective_id=0, has_side_effects=True, vmem_limit_bytes=58 * 2**20),
        )(lengthscale, outscale, x_loc, v_loc.T)
        return y_t.T

    return jax.shard_map(local_fn, mesh=mesh, in_specs=(row_spec, row_spec, P(None), P(None)), out_specs=row_spec, check_vma=False)
```
